8 devices in a mesh: data: 1 (over z), model: 2 (over y), time: 4 (over x, core).
Axes of the slice: x: 2, y: 2, z: 1, core: 2. Of those that a mesh axis runs over, the one named last changes fastest.
Arguments:
- x_init: float32 [4, 1024, 16], P('data')
- w_up: bfloat16 [16, 1152], P(None, 'model')
- w_down: bfloat16 [1152, 16], P('model')
- mod_scale: bfloat16 [8, 1152], P('time', 'model')
- mod_shift: bfloat16 [8, 1152], P('time', 'model')
- step_size: float32 [8], P('time')
Outputs:
- output: float32 [8, 4, 1024, 16], P('time', 'data')
All inputs are finite; a program needn't handle non-finite values.
Results may differ from the reference program's by a relative error of at most 0.001.
Values are sent between devices in bfloat16 or wider.
A program may use at most 1 GiB of HBM per device.

```python
import jax
import jax.numpy as jnp
from jax import lax

STEPS = 8
BATCH = 4
TOKENS = 1024
CHAN = 16
HIDDEN = 1152
SWEEPS = 4


def setup_inputs(seed: int = 0, part: int = 0) -> dict:
    base_key = jax.random.key(seed)
    key_list = jax.random.split(base_key, 6)
    part_key = jax.random.fold_in(key_list[5], part)
    x_init = jax.random.normal(part_key, (BATCH, TOKENS, CHAN), jnp.float32)
    w_up = (jax.random.normal(key_list[0], (CHAN, HIDDEN), jnp.float32) * CHAN ** -0.5).astype(jnp.bfloat16)
    w_down = (jax.random.normal(key_list[1], (HIDDEN, CHAN), jnp.float32) * HIDDEN ** -0.5).astype(jnp.bfloat16)
    mod_scale = (0.5 * jax.random.normal(key_list[2], (STEPS, HIDDEN), jnp.float32)).astype(jnp.bfloat16)
    mod_shift = (0.5 * jax.random.normal(key_list[3], (STEPS, HIDDEN), jnp.float32)).astype(jnp.bfloat16)
    step_size = (3.0 / STEPS) * jax.random.uniform(key_list[4], (STEPS,), jnp.float32, 0.2, 1.8)
    return {'x_init': x_init, 'w_up': w_up, 'w_down': w_down, 'mod_scale': mod_scale, 'mod_shift': mod_shift, 'step_size': step_size}


def drift_at(latent, scale_row, shift_row, step_val, w_up, w_down):
    flat_lat = latent.reshape(BATCH * TOKENS, CHAN).astype(jnp.bfloat16)
    pre_act = jnp.dot(flat_lat, w_up, preferred_element_type=jnp.float32)
    hidden = jax.nn.gelu(pre_act * (1.0 + scale_row.astype(jnp.float32)) + shift_row.astype(jnp.float32), approximate=True)
    proj_out = jnp.dot(hidden.astype(jnp.bfloat16), w_down, preferred_element_type=jnp.float32)
    return step_val * proj_out.reshape(BATCH, TOKENS, CHAN)


def reference(x_init, w_up, w_down, mod_scale, mod_shift, step_size):
    def drift_step(packed):
        return drift_at(packed[0], packed[1], packed[2], packed[3], w_up, w_down)

    def one_sweep(latents, unused):
        drifts = lax.map(drift_step, (latents, mod_scale, mod_shift, step_size))
        prefix = jnp.cumsum(drifts, axis=0) - drifts
        return x_init[None] + prefix, unused

    start_lat = jnp.broadcast_to(x_init[None], (STEPS, BATCH, TOKENS, CHAN))
    final_lat, unused = lax.scan(one_sweep, start_lat, None, length=SWEEPS)
    return final_lat
```

```python
import functools

import jax
import jax.numpy as jnp
from jax import lax
from jax.experimental import pallas as pl
from jax.experimental.pallas import tpu as pltpu
from jax.sharding import PartitionSpec as P

MESH = pl.DeviceIdType.MESH
SWEEPS = 4
STEPS = 8
NM, NT = 2, 4
BATCH, TOKENS, CHAN = 4, 1024, 16
HALF = 576
BODY = 512
HIDDEN = 2 * HALF
DEV_TOK = BATCH * TOKENS // (NM * NT)
CHUNKS = 2
TM = DEV_TOK // CHUNKS
ROW = 640
HID_TILE = 256
TANH_LIN = 0.7978845608028654
TANH_CUB = TANH_LIN * 0.044715


def twice_gelu_half(half):
    inner = half * ((8.0 * TANH_CUB) * (half * half) + 2.0 * TANH_LIN)
    return half * jnp.tanh(inner) + half


def drift(x_rows, step, w_up, w_down_t, scale, shift):
    total = None
    for lo in range(0, HIDDEN, HID_TILE):
        cols = slice(lo, min(lo + HID_TILE, HIDDEN))
        pre = jnp.dot(x_rows, w_up[:, cols], preferred_element_type=jnp.float32)
        hidden = twice_gelu_half(pre * scale[step:step + 1, cols] + shift[step:step + 1, cols])
        part = lax.dot_general(w_down_t[:, cols], hidden.astype(jnp.bfloat16), (((1,), (1,)), ((), ())),
                               preferred_element_type=jnp.float32)
        total = part if total is None else total + part
    return total


def join_halves(a, b):
    return jnp.concatenate([a[:, :BODY], b[:, :BODY], a[:, BODY:HALF], b[:, BODY:HALF]], axis=1)


def kernel(x_ref, up_ref, down_ref, gam_ref, bet_ref, step_ref, out_ref,
           x0, up_half, down_half, row_loc, rows, w_up, w_down_t, scale, shift, final,
           loc_sem, psend, precv, wsend, wrecv, osend, orecv):
    me_m = lax.axis_index("model")
    me_t = lax.axis_index("time")
    me = me_m * NT + me_t
    sample = me // 2
    tok0 = pl.multiple_of((me % 2) * DEV_TOK, DEV_TOK)

    def peer(dm, dt):
        return (0, (me_m + dm) % NM, (me_t + dt) % NT)

    others = [(dm, dt) for dm in range(NM) for dt in range(NT) if (dm, dt) != (0, 0)]

    barrier = pltpu.get_barrier_semaphore()
    for dm, dt in others:
        pl.semaphore_signal(barrier, inc=1, device_id=peer(dm, dt), device_id_type=MESH)

    x_copy = pltpu.make_async_copy(x_ref.at[sample, :, pl.ds(tok0, DEV_TOK)], x0, loc_sem.at[0])
    x_copy.start()

    row_loc[0:2, 0:HALF] = 0.5 * (1.0 + gam_ref[...].astype(jnp.float32))
    row_loc[2:4, 0:HALF] = 0.5 * bet_ref[...].astype(jnp.float32)
    for r in range(2):
        row_loc[r:r + 1, HALF:ROW] = jnp.full((1, ROW - HALF), step_ref[r], jnp.float32)
    rows[me_m, me_t] = row_loc[...]
    up_half[me_m] = up_ref[...]
    down_half[me_m] = down_ref[...]

    pl.semaphore_wait(barrier, len(others))

    sends = []
    for n, (dm, dt) in enumerate(others):
        copy = pltpu.make_async_remote_copy(row_loc, rows.at[me_m, me_t], psend.at[n], precv.at[n],
                                            device_id=peer(dm, dt), device_id_type=MESH)
        copy.start()
        sends.append(copy)
    for n, (src, dst) in enumerate(((up_ref, up_half), (down_ref, down_half))):
        copy = pltpu.make_async_remote_copy(src, dst.at[me_m], wsend.at[n], wrecv.at[n],
                                            device_id=peer(1, 0), device_id_type=MESH)
        copy.start()
        sends.append(copy)
    for copy in sends:
        copy.wait_recv()
    x_copy.wait()

    @pl.when(me_t == 0)
    def _():
        copy = pltpu.make_async_copy(x_ref, out_ref.at[0], loc_sem.at[1])
        copy.start()
        copy.wait()

    w_up[...] = join_halves(up_half[0], up_half[1])
    w_down_t[...] = join_halves(down_half[0], down_half[1])
    for t in range(NT):
        scale[2 * t:2 * t + 2, :] = join_halves(rows[0, t, 0:2, :], rows[1, t, 0:2, :])
        shift[2 * t:2 * t + 2, :] = join_halves(rows[0, t, 2:4, :], rows[1, t, 2:4, :])

    out_copies = []

    def place(j, c):
        return out_ref.at[j % 2, sample, :, pl.ds(pl.multiple_of(tok0 + c * TM, TM), TM)]

    def publish(j, c, value):
        owner = j // 2
        src = final.at[c, j]
        src[...] = value
        dt = (owner + NT - me_t) % NT
        far = pltpu.make_async_remote_copy(src, place(j, c), osend.at[j, c, 0], orecv.at[1, dt, j % 2, c],
                                           device_id=(0, (me_m + 1) % NM, owner), device_id_type=MESH)
        far.start()
        near = pltpu.make_async_remote_copy(src, place(j, c), osend.at[j, c, 1], orecv.at[0, dt, j % 2, c],
                                            device_id=(0, me_m, owner), device_id_type=MESH)
        out_copies.append((owner, far, near))

        @pl.when(me_t != owner)
        def _():
            near.start()

        @pl.when(me_t == owner)
        def _():
            place(j, c)[...] = value

    for c in range(CHUNKS):
        start = x0[:, c * TM:(c + 1) * TM]
        latents = {j: start for j in range(SWEEPS)}
        settled = jnp.zeros_like(start)
        for sweep in range(1, SWEEPS + 1):
            running = settled
            fresh = {}
            for j in range(sweep - 1, sweep + 3):
                value = drift(latents[j].T.astype(jnp.bfloat16), j, w_up, w_down_t, scale, shift)
                running = running + rows[0, j // 2, j % 2:j % 2 + 1, HALF:HALF + 1] * value
                fresh[j + 1] = start + running
                if j == sweep - 1:
                    settled = running
                if j == sweep - 1 or sweep == SWEEPS:
                    publish(j + 1, c, fresh[j + 1])
            latents = fresh

    for copy in sends:
        copy.wait_send()
    for owner, far, near in out_copies:
        far.wait_send()

        @pl.when(me_t != owner)
        def _():
            near.wait_send()

    for r in range(2):
        def arrivals():
            for dm, dt in others:
                for c in range(CHUNKS):
                    pltpu.make_async_remote_copy(final.at[c, r], place(r, c), osend.at[0, 0, 0], orecv.at[dm, dt, r, c],
                                                 device_id=peer(dm, dt), device_id_type=MESH).wait_recv()
        if r == 0:
            pl.when(me_t > 0)(arrivals)
        else:
            arrivals()


def solution(mesh):
    def device_body(x_init, w_up, w_down, mod_scale, mod_shift, step_size):
        x_t = jnp.swapaxes(x_init, 1, 2)
        vmem = pl.BlockSpec(memory_space=pltpu.VMEM)
        out = pl.pallas_call(
            kernel,
            out_shape=jax.ShapeDtypeStruct((2, BATCH, CHAN, TOKENS), jnp.float32),
            in_specs=[pl.BlockSpec(memory_space=pl.ANY), vmem, vmem, vmem, vmem, pl.BlockSpec(memory_space=pltpu.SMEM)],
            out_specs=vmem,
            scratch_shapes=[
                pltpu.VMEM((CHAN, DEV_TOK), jnp.float32),
                pltpu.VMEM((NM, CHAN, HALF), jnp.bfloat16),
                pltpu.VMEM((NM, CHAN, HALF), jnp.bfloat16),
                pltpu.VMEM((4, ROW), jnp.float32),
                pltpu.VMEM((NM, NT, 4, ROW), jnp.float32),
                pltpu.VMEM((CHAN, HIDDEN), jnp.bfloat16),
                pltpu.VMEM((CHAN, HIDDEN), jnp.bfloat16),
                pltpu.VMEM((STEPS, HIDDEN), jnp.float32),
                pltpu.VMEM((STEPS, HIDDEN), jnp.float32),
                pltpu.VMEM((CHUNKS, STEPS, CHAN, TM), jnp.float32),
                pltpu.SemaphoreType.DMA((2,)),
                pltpu.SemaphoreType.DMA((7,)),
                pltpu.SemaphoreType.DMA((7,)),
                pltpu.SemaphoreType.DMA((2,)),
                pltpu.SemaphoreType.DMA((2,)),
                pltpu.SemaphoreType.DMA((STEPS, CHUNKS, 2)),
                pltpu.SemaphoreType.DMA((NM, NT, 2, CHUNKS)),
            ],
            compiler_params=pltpu.CompilerParams(collective_id=0, has_side_effects=True),
        )(x_t, w_up, w_down.T, mod_scale, mod_shift, step_size)
        return jnp.swapaxes(out, 2, 3)

    return jax.shard_map(device_body, mesh=mesh, in_specs=(P('data', None, None), P(None, 'model'), P('model', None), P('time', 'model'), P('time', 'model'), P('time')), out_specs=P('time', 'data', None, None), check_vma=False)
```

```python
import jax
import jax.numpy as jnp
from jax import lax
from jax.experimental import pallas as pl
from jax.experimental.pallas import tpu as pltpu
from jax.sharding import PartitionSpec as P

MESH = pl.DeviceIdType.MESH
SWEEPS = 4
STEPS = 8
NM, NT = 2, 4
BATCH, TOKENS, CHAN = 4, 1024, 16
HALF = 576
BODY = 512
HIDDEN = 2 * HALF
DEV_TOK = BATCH * TOKENS // (NM * NT)
CHUNKS = 2
TM = DEV_TOK // CHUNKS
HID_TILE = 1152
TANH_LIN = 0.7978845608028654
TANH_CUB = TANH_LIN * 0.044715


def gelu_from_half(half):
    inner = half * ((8.0 * TANH_CUB) * (half * half) + 2.0 * TANH_LIN)
    return half * jnp.tanh(inner) + half


def drift(x_rows, scale_row, shift_row, w_up, w_down_t, lo, hi, tile=HID_TILE):
    total = None
    for at in range(lo, hi, tile):
        cols = slice(at, min(at + tile, hi))
        pre = jnp.dot(x_rows, w_up[:, cols], preferred_element_type=jnp.float32)
        hidden = gelu_from_half(pre * scale_row[:, cols] + shift_row[:, cols])
        part = lax.dot_general(w_down_t[:, cols], hidden.astype(jnp.bfloat16), (((1,), (1,)), ((), ())),
                               preferred_element_type=jnp.float32)
        total = part if total is None else total + part
    return total


def kernel(x_ref, up_ref, down_ref, gam_ref, bet_ref, step_ref, out_ref,
           x0, w_own, w_other, rows, steps, w_up, w_down_t, scale, shift, first, final,
           loc_sem, rsend, rrecv, hsend, hrecv, wsend, wrecv, osend, orecv):
    me_m = lax.axis_index("model")
    me_t = lax.axis_index("time")
    me = me_m * NT + me_t
    sample = me // 2
    tok0 = pl.multiple_of((me % 2) * DEV_TOK, DEV_TOK)

    def peer(dm, dt):
        return (0, (me_m + dm) % NM, (me_t + dt) % NT)

    others = [(dm, dt) for dm in range(NM) for dt in range(NT) if (dm, dt) != (0, 0)]

    barrier = pltpu.get_barrier_semaphore()
    for dm, dt in others:
        pl.semaphore_signal(barrier, inc=1, device_id=peer(dm, dt), device_id_type=MESH)

    local = [pltpu.make_async_copy(src, dst, loc_sem.at[n]) for n, (src, dst) in enumerate((
        (gam_ref, rows.at[0, me_t, 0]), (bet_ref, rows.at[0, me_t, 1]), (up_ref, w_own.at[0]), (down_ref, w_own.at[1]),
        (x_ref.at[sample, :, pl.ds(tok0, DEV_TOK)], x0), (step_ref, steps.at[me_t])))]
    for copy in local:
        copy.start()
    keep = pltpu.make_async_copy(x_ref, out_ref.at[0], loc_sem.at[6])

    @pl.when(me_t == 0)
    def _():
        keep.start()

    for copy in local:
        copy.wait()

    def table(half, t, cols, src):
        scale[t, :, cols] = 0.5 * (1.0 + rows[half, t, 0].astype(jnp.float32)[:, src])
        shift[t, :, cols] = 0.5 * rows[half, t, 1].astype(jnp.float32)[:, src]

    own_cols = slice(0, BODY)

    def first_pair(t):
        table(0, t, own_cols, own_cols)
        for r in range(2):
            for c in range(CHUNKS):
                tok = slice(c * TM, (c + 1) * TM)
                first[t, r, :, tok] = drift(x0[:, tok].T.astype(jnp.bfloat16), scale[t, r:r + 1, :], shift[t, r:r + 1, :],
                                            w_up, w_down_t, 0, BODY)

    w_up[:, own_cols] = w_own[0][:, own_cols]
    w_down_t[:, own_cols] = w_own[1][:, own_cols]

    @pl.when(me_t < 2)
    def _():
        first_pair(me_t)

    pl.semaphore_wait(barrier, len(others))

    sends = []

    def send(src, dst, ssem, rsem, to):
        copy = pltpu.make_async_remote_copy(src, dst, ssem, rsem, device_id=to, device_id_type=MESH)
        copy.start()
        sends.append(copy)

    def arrived(buf, sem):
        pltpu.make_async_remote_copy(buf, buf, rsend.at[0, 0], sem, device_id=peer(1, 0), device_id_type=MESH).wait_recv()

    mine = rows.at[0, me_t]
    for dt in (2, 3, 1):
        send(mine, mine, rsend.at[0, dt], rrecv.at[0, me_t], peer(0, dt))
    for dt in (2, 3, 1, 0):
        send(mine, rows.at[1, me_t], rsend.at[1, dt], rrecv.at[1, me_t], peer(1, dt))
    send(w_own, w_other, wsend, wrecv, peer(1, 0))
    for dt in (2, 3, 1):
        send(steps.at[me_t], steps.at[me_t], hsend.at[dt], hrecv.at[me_t], peer(0, dt))

    def rows_arrived(half, t):
        if half == 1:
            arrived(rows.at[1, t], rrecv.at[1, t])
        else:
            @pl.when(me_t != t)
            def _():
                arrived(rows.at[0, t], rrecv.at[0, t])

    rows_arrived(0, 0)
    rows_arrived(0, 1)
    first_pair(jnp.where(me_t < 2, 1 - me_t, 0))

    @pl.when(me_t >= 2)
    def _():
        first_pair(1)

    arrived(w_other, wrecv)
    rows_arrived(1, 0)
    rows_arrived(1, 1)

    other_cols = slice(BODY, 2 * BODY)
    rest = slice(BODY, HALF)
    rest_cols = slice(2 * BODY, HIDDEN)

    def join(a, b):
        return jnp.concatenate([a[:, rest], b[:, rest]], axis=1)

    for n, dst in enumerate((w_up, w_down_t)):
        dst[:, other_cols] = w_other[n][:, own_cols]
        dst[:, rest_cols] = join(w_own[n], w_other[n])

    def finish_table(t):
        table(1, t, other_cols, own_cols)
        scale[t, :, rest_cols] = 0.5 * (1.0 + join(rows[0, t, 0].astype(jnp.float32), rows[1, t, 0].astype(jnp.float32)))
        shift[t, :, rest_cols] = 0.5 * join(rows[0, t, 1].astype(jnp.float32), rows[1, t, 1].astype(jnp.float32))

    for t in range(2):
        finish_table(t)

    def evaluate(latent, j, lo):
        return drift(latent.T.astype(jnp.bfloat16), scale[j // 2, j % 2:j % 2 + 1, :], shift[j // 2, j % 2:j % 2 + 1, :],
                     w_up, w_down_t, lo, HIDDEN)

    def step_value(j):
        return steps[j // 2, :, j % 2:j % 2 + 1]

    out_copies = []

    def place(j, c):
        return out_ref.at[j % 2, sample, :, pl.ds(pl.multiple_of(tok0 + c * TM, TM), TM)]

    def publish(j, c, value):
        owner = j // 2
        src = final.at[c, j]
        src[...] = value
        dt = (owner + NT - me_t) % NT
        far = pltpu.make_async_remote_copy(src, place(j, c), osend.at[j, c, 0], orecv.at[1, dt, j % 2, c],
                                           device_id=(0, (me_m + 1) % NM, owner), device_id_type=MESH)
        far.start()
        near = pltpu.make_async_remote_copy(src, place(j, c), osend.at[j, c, 1], orecv.at[0, dt, j % 2, c],
                                            device_id=(0, me_m, owner), device_id_type=MESH)
        out_copies.append((owner, far, near))

        @pl.when(me_t != owner)
        def _():
            near.start()

    starts = [x0[:, c * TM:(c + 1) * TM] for c in range(CHUNKS)]
    settled = [None] * CHUNKS
    running = [None] * CHUNKS

    def sweep_step(sweep, j, c, value):
        value = step_value(j) * value
        if j == sweep - 1:
            running[c] = settled[c]
        running[c] = value if running[c] is None else running[c] + value
        fresh[c][j + 1] = starts[c] + running[c]
        if j == sweep - 1:
            settled[c] = running[c]
        if j == sweep - 1 or sweep == SWEEPS:
            publish(j + 1, c, fresh[c][j + 1])

    for t in range(2):
        @pl.when(me_t != t)
        def _():
            arrived(steps.at[t], hrecv.at[t])
    fresh = [{} for _ in range(CHUNKS)]
    for j in range(SWEEPS):
        for c in range(CHUNKS):
            value = first[j // 2, j % 2, :, c * TM:(c + 1) * TM] + evaluate(starts[c], j, BODY)
            sweep_step(1, j, c, value)

    for t in range(2, NT):
        rows_arrived(0, t)
        rows_arrived(1, t)

        @pl.when(me_t != t)
        def _():
            arrived(steps.at[t], hrecv.at[t])

        table(0, t, own_cols, own_cols)
        finish_table(t)

    latents = [None] * CHUNKS
    for c, n in ORDER:
        sweep, j = n // 4 + 1, n // 4 + n % 4
        if n % 4 == 0:
            latents[c] = fresh[c]
            fresh[c] = {}
        sweep_step(sweep, j, c, evaluate(latents[c][j], j, 0))

    for j in range(1, STEPS):
        @pl.when(me_t == j // 2)
        def _():
            for c in range(CHUNKS):
                place(j, c)[...] = final[c, j]

    for copy in sends:
        copy.wait_send()
    for owner, far, near in out_copies:
        far.wait_send()

        @pl.when(me_t != owner)
        def _():
            near.wait_send()

    @pl.when(me_t == 0)
    def _():
        keep.wait()

    for r in range(2):
        def arrivals():
            for dm, dt in others:
                for c in range(CHUNKS):
                    arrived(place(r, c), orecv.at[dm, dt, r, c])
        if r == 0:
            pl.when(me_t > 0)(arrivals)
        else:
            arrivals()


ORDER = [(c, n) for c in range(CHUNKS) for n in range(4, 16)]


def solution(mesh):
    def device_body(x_init, w_up, w_down, mod_scale, mod_shift, step_size):
        x_t = jnp.swapaxes(x_init, 1, 2)
        anywhere = pl.BlockSpec(memory_space=pl.ANY)
        out = pl.pallas_call(
            kernel,
            out_shape=pltpu.VMEM((2, BATCH, CHAN, TOKENS), jnp.float32),
            in_specs=[anywhere] * 6,
            out_specs=pl.BlockSpec(memory_space=pltpu.VMEM),
            scratch_shapes=[
                pltpu.VMEM((CHAN, DEV_TOK), jnp.float32),
                pltpu.VMEM((2, CHAN, HALF), jnp.bfloat16),
                pltpu.VMEM((2, CHAN, HALF), jnp.bfloat16),
                pltpu.VMEM((NM, NT, 2, 2, HALF), jnp.bfloat16),
                pltpu.VMEM((NT, 1, 2), jnp.float32),
                pltpu.VMEM((CHAN, HIDDEN), jnp.bfloat16),
                pltpu.VMEM((CHAN, HIDDEN), jnp.bfloat16),
                pltpu.VMEM((NT, 2, HIDDEN), jnp.float32),
                pltpu.VMEM((NT, 2, HIDDEN), jnp.float32),
                pltpu.VMEM((2, 2, CHAN, DEV_TOK), jnp.float32),
                pltpu.VMEM((CHUNKS, STEPS, CHAN, TM), jnp.float32),
                pltpu.SemaphoreType.DMA((7,)),
                pltpu.SemaphoreType.DMA((NM, NT)),
                pltpu.SemaphoreType.DMA((NM, NT)),
                pltpu.SemaphoreType.DMA((NT,)),
                pltpu.SemaphoreType.DMA((NT,)),
                pltpu.SemaphoreType.DMA,
                pltpu.SemaphoreType.DMA,
                pltpu.SemaphoreType.DMA((STEPS, CHUNKS, 2)),
                pltpu.SemaphoreType.DMA((NM, NT, 2, CHUNKS)),
            ],
            compiler_params=pltpu.CompilerParams(collective_id=0, has_side_effects=True),
        )(x_t, w_up, w_down.T, mod_scale, mod_shift, step_size.reshape(1, 2))
        return jnp.swapaxes(out, 2, 3)

    return jax.shard_map(device_body, mesh=mesh, in_specs=(P('data', None, None), P(None, 'model'), P('model', None), P('time', 'model'), P('time', 'model'), P('time')), out_specs=P('time', 'data', None, None), check_vma=False)
```

```python
import jax
import jax.numpy as jnp
from jax import lax
from jax.experimental import pallas as pl
from jax.experimental.pallas import tpu as pltpu
from jax.sharding import PartitionSpec as P

MESH = pl.DeviceIdType.MESH
SWEEPS = 4
STEPS = 8
NM, NT = 2, 4
BATCH, TOKENS, CHAN = 4, 1024, 16
HALF = 576
BODY = 512
HIDDEN = 2 * HALF
DEV_TOK = BATCH * TOKENS // (NM * NT)
CHUNKS = 2
TM = DEV_TOK // CHUNKS
HID_TILE = 256
LOOK, LAG = 2, 1
TANH_LIN = 0.7978845608028654
TANH_CUB = TANH_LIN * 0.044715


def gelu_from_half(half):
    inner = half * ((8.0 * TANH_CUB) * (half * half) + 2.0 * TANH_LIN)
    return half * jnp.tanh(inner) + half


def emit(units, w_up, w_down_t):
    blocks = [(u, at, min(at + HID_TILE, u[3][1])) for u in units for at in range(u[3][0], u[3][1], HID_TILE)]
    rows, pre, hidden, totals = {}, {}, {}, {}

    def up(n):
        unit, lo, hi = blocks[n]
        if lo == unit[3][0]:
            rows[id(unit)] = unit[0]().T.astype(jnp.bfloat16)
        pre[n] = jnp.dot(rows[id(unit)], w_up[:, lo:hi], preferred_element_type=jnp.float32)

    def act(n):
        unit, lo, hi = blocks[n]
        hidden[n] = gelu_from_half(pre.pop(n) * unit[1](lo, hi) + unit[2](lo, hi)).astype(jnp.bfloat16)

    def down(n):
        unit, lo, hi = blocks[n]
        part = lax.dot_general(w_down_t[:, lo:hi], hidden.pop(n), (((1,), (1,)), ((), ())),
                               preferred_element_type=jnp.float32)
        totals[id(unit)] = part if lo == unit[3][0] else totals[id(unit)] + part
        if hi == unit[3][1]:
            unit[4](totals.pop(id(unit)))

    for n in range(min(LOOK, len(blocks))):
        up(n)
    for n in range(len(blocks)):
        if n + LOOK < len(blocks):
            up(n + LOOK)
        act(n)
        if n >= LAG:
            down(n - LAG)
    for n in range(max(0, len(blocks) - LAG), len(blocks)):
        down(n)


def kernel(x_ref, up_ref, down_ref, gam_ref, bet_ref, step_ref, out_ref,
           x0, w_own, w_other, rows, steps, w_up, w_down_t, scale, shift, first, final, tally,
           loc_sem, rsend, rrecv, hsend, hrecv, wsend, wrecv, osend, orecv):
    me_m = lax.axis_index("model")
    me_t = lax.axis_index("time")
    me = me_m * NT + me_t
    sample = me // 2
    tok0 = pl.multiple_of((me % 2) * DEV_TOK, DEV_TOK)

    def peer(dm, dt):
        return (0, (me_m + dm) % NM, (me_t + dt) % NT)

    others = [(dm, dt) for dm in range(NM) for dt in range(NT) if (dm, dt) != (0, 0)]

    barrier = pltpu.get_barrier_semaphore()
    for dm, dt in others:
        pl.semaphore_signal(barrier, inc=1, device_id=peer(dm, dt), device_id_type=MESH)

    local = [pltpu.make_async_copy(src, dst, loc_sem.at[n]) for n, (src, dst) in enumerate((
        (gam_ref, rows.at[0, me_t, 0]), (bet_ref, rows.at[0, me_t, 1]), (up_ref, w_own.at[0]), (down_ref, w_own.at[1]),
        (x_ref.at[sample, :, pl.ds(tok0, DEV_TOK)], x0), (step_ref, steps.at[me_t])))]
    for copy in local:
        copy.start()
    keep = pltpu.make_async_copy(x_ref, out_ref.at[0], loc_sem.at[6])

    @pl.when(me_t == 0)
    def _():
        keep.start()

    for copy in local:
        copy.wait()

    def table(half, t, cols, src):
        scale[t, :, cols] = 0.5 * (1.0 + rows[half, t, 0].astype(jnp.float32)[:, src])
        shift[t, :, cols] = 0.5 * rows[half, t, 1].astype(jnp.float32)[:, src]

    own_cols = slice(0, BODY)

    def first_pair(t):
        table(0, t, own_cols, own_cols)

        def unit(r, c):
            tok = slice(c * TM, (c + 1) * TM)

            def done(total):
                first[t, r, :, tok] = total
            return (lambda: x0[:, tok], lambda lo, hi: scale[t, r:r + 1, lo:hi], lambda lo, hi: shift[t, r:r + 1, lo:hi],
                    (0, BODY), done)
        emit([unit(r, c) for r in range(2) for c in range(CHUNKS)], w_up, w_down_t)

    w_up[:, own_cols] = w_own[0][:, own_cols]
    w_down_t[:, own_cols] = w_own[1][:, own_cols]

    @pl.when(me_t < 2)
    def _():
        first_pair(me_t)

    pl.semaphore_wait(barrier, len(others))

    sends = []

    def send(src, dst, ssem, rsem, to):
        copy = pltpu.make_async_remote_copy(src, dst, ssem, rsem, device_id=to, device_id_type=MESH)
        copy.start()
        sends.append(copy)

    def arrived(buf, sem):
        pltpu.make_async_remote_copy(buf, buf, rsend.at[0, 0], sem, device_id=peer(1, 0), device_id_type=MESH).wait_recv()

    mine = rows.at[0, me_t]
    for dt in (2, 3, 1):
        send(mine, mine, rsend.at[0, dt], rrecv.at[0, me_t], peer(0, dt))
    for dt in (2, 3, 1, 0):
        send(mine, rows.at[1, me_t], rsend.at[1, dt], rrecv.at[1, me_t], peer(1, dt))
    send(w_own, w_other, wsend, wrecv, peer(1, 0))
    for dt in (2, 3, 1):
        send(steps.at[me_t], steps.at[me_t], hsend.at[dt], hrecv.at[me_t], peer(0, dt))

    def rows_arrived(half, t):
        if half == 1:
            arrived(rows.at[1, t], rrecv.at[1, t])
        else:
            @pl.when(me_t != t)
            def _():
                arrived(rows.at[0, t], rrecv.at[0, t])

    rows_arrived(0, 0)
    rows_arrived(0, 1)
    first_pair(jnp.where(me_t < 2, 1 - me_t, 0))

    @pl.when(me_t >= 2)
    def _():
        first_pair(1)

    arrived(w_other, wrecv)
    for t in range(NT):
        if t > 1:
            rows_arrived(0, t)
        rows_arrived(1, t)

        @pl.when(me_t != t)
        def _():
            arrived(steps.at[t], hrecv.at[t])

    other_cols = slice(BODY, 2 * BODY)
    rest = slice(BODY, HALF)
    rest_cols = slice(2 * BODY, HIDDEN)

    def join(a, b):
        return jnp.concatenate([a[:, rest], b[:, rest]], axis=1)

    for n, dst in enumerate((w_up, w_down_t)):
        dst[:, other_cols] = w_other[n][:, own_cols]
        dst[:, rest_cols] = join(w_own[n], w_other[n])

    def finish_table(t):
        table(1, t, other_cols, own_cols)
        scale[t, :, rest_cols] = 0.5 * (1.0 + join(rows[0, t, 0].astype(jnp.float32), rows[1, t, 0].astype(jnp.float32)))
        shift[t, :, rest_cols] = 0.5 * join(rows[0, t, 1].astype(jnp.float32), rows[1, t, 1].astype(jnp.float32))

    for t in range(NT):
        if t > 1:
            table(0, t, own_cols, own_cols)
        finish_table(t)

    def step_value(j):
        return steps[j // 2, :, j % 2:j % 2 + 1]

    def place(j, c):
        return out_ref.at[j % 2, sample, :, pl.ds(pl.multiple_of(tok0 + c * TM, TM), TM)]

    def publish(j, c, value):
        owner = j // 2
        src = final.at[c, j]
        src[...] = value
        far = pltpu.make_async_remote_copy(src, place(j, c), osend.at[0], orecv.at[j % 2],
                                           device_id=(0, (me_m + 1) % NM, owner), device_id_type=MESH)
        far.start()
        near = pltpu.make_async_remote_copy(src, place(j, c), osend.at[1 + owner], orecv.at[j % 2],
                                            device_id=(0, me_m, owner), device_id_type=MESH)

        @pl.when(me_t != owner)
        def _():
            near.start()

    latents = {}
    settled, running = {}, {}

    def unit(sweep, j, c):
        tok = slice(c * TM, (c + 1) * TM)

        def latent():
            return x0[:, tok] if sweep == 1 else latents[sweep - 1, j, c]

        def done(total):
            if sweep == 1:
                total = first[j // 2, j % 2, :, tok] + total
            value = step_value(j) * total
            base = running[c] if j > sweep - 1 else settled.get(c)
            running[c] = value if base is None else base + value
            latents[sweep, j + 1, c] = x0[:, tok] + running[c]
            if j == sweep - 1:
                settled[c] = running[c]
            if j == sweep - 1 or sweep == SWEEPS:
                publish(j + 1, c, latents[sweep, j + 1, c])
        row = slice(j % 2, j % 2 + 1)
        return (latent, lambda lo, hi: scale[j // 2, row, lo:hi], lambda lo, hi: shift[j // 2, row, lo:hi],
                (BODY if sweep == 1 else 0, HIDDEN), done)

    emit([unit(sweep, j, c) for c in range(CHUNKS) for sweep in range(1, SWEEPS + 1) for j in range(sweep - 1, sweep + 3)],
         w_up, w_down_t)

    for j in range(1, STEPS):
        @pl.when(me_t == j // 2)
        def _():
            for c in range(CHUNKS):
                place(j, c)[...] = final[c, j]

    for copy in sends:
        copy.wait_send()
    def drained(sem, count):
        pltpu.make_async_copy(tally.at[pl.ds(0, count)], tally.at[pl.ds(0, count)], sem).wait()

    drained(osend.at[0], CHUNKS * (STEPS - 1))
    for owner in range(NT):
        @pl.when(me_t != owner)
        def _():
            drained(osend.at[1 + owner], CHUNKS * (2 if owner else 1))

    @pl.when(me_t == 0)
    def _():
        keep.wait()

    @pl.when(me_t > 0)
    def _():
        drained(orecv.at[0], CHUNKS * len(others))

    drained(orecv.at[1], CHUNKS * len(others))


def solution(mesh):
    def device_body(x_init, w_up, w_down, mod_scale, mod_shift, step_size):
        x_t = jnp.swapaxes(x_init, 1, 2)
        anywhere = pl.BlockSpec(memory_space=pl.ANY)
        out = pl.pallas_call(
            kernel,
            out_shape=pltpu.VMEM((2, BATCH, CHAN, TOKENS), jnp.float32),
            in_specs=[anywhere] * 6,
            out_specs=pl.BlockSpec(memory_space=pltpu.VMEM),
            scratch_shapes=[
                pltpu.VMEM((CHAN, DEV_TOK), jnp.float32),
                pltpu.VMEM((2, CHAN, HALF), jnp.bfloat16),
                pltpu.VMEM((2, CHAN, HALF), jnp.bfloat16),
                pltpu.VMEM((NM, NT, 2, 2, HALF), jnp.bfloat16),
                pltpu.VMEM((NT, 1, 2), jnp.float32),
                pltpu.VMEM((CHAN, HIDDEN), jnp.bfloat16),
                pltpu.VMEM((CHAN, HIDDEN), jnp.bfloat16),
                pltpu.VMEM((NT, 2, HIDDEN), jnp.float32),
                pltpu.VMEM((NT, 2, HIDDEN), jnp.float32),
                pltpu.VMEM((2, 2, CHAN, DEV_TOK), jnp.float32),
                pltpu.VMEM((CHUNKS, STEPS, CHAN, TM), jnp.float32),
                pltpu.VMEM((CHUNKS * (STEPS - 1), CHAN, TM), jnp.float32),
                pltpu.SemaphoreType.DMA((7,)),
                pltpu.SemaphoreType.DMA((NM, NT)),
                pltpu.SemaphoreType.DMA((NM, NT)),
                pltpu.SemaphoreType.DMA((NT,)),
                pltpu.SemaphoreType.DMA((NT,)),
                pltpu.SemaphoreType.DMA,
                pltpu.SemaphoreType.DMA,
                pltpu.SemaphoreType.DMA((1 + NT,)),
                pltpu.SemaphoreType.DMA((2,)),
            ],
            compiler_params=pltpu.CompilerParams(collective_id=0, has_side_effects=True),
        )(x_t, w_up, w_down.T, mod_scale, mod_shift, step_size.reshape(1, 2))
        return jnp.swapaxes(out, 2, 3)

    return jax.shard_map(device_body, mesh=mesh, in_specs=(P('data', None, None), P(None, 'model'), P('model', None), P('time', 'model'), P('time', 'model'), P('time')), out_specs=P('time', 'data', None, None), check_vma=False)
```

```python
import jax
import jax.numpy as jnp
from jax import lax
from jax.experimental import pallas as pl
from jax.experimental.pallas import tpu as pltpu
from jax.sharding import PartitionSpec as P

MESH = pl.DeviceIdType.MESH
SWEEPS = 4
STEPS = 8
NM, NT = 2, 4
BATCH, TOKENS, CHAN = 4, 1024, 16
HALF = 576
BODY = 512
HIDDEN = 2 * HALF
DEV_TOK = BATCH * TOKENS // (NM * NT)
CHUNKS = 2
TM = DEV_TOK // CHUNKS
HID_TILE = 256
LOOK, LAG = 1, 1
SEND_AFTER = {1: 1, 3: 2, 5: 4, 7: 6}
TANH_LIN = 0.7978845608028654
TANH_CUB = TANH_LIN * 0.044715


def gelu_from_half(half):
    inner = half * ((8.0 * TANH_CUB) * (half * half) + 2.0 * TANH_LIN)
    return half * jnp.tanh(inner) + half


def emit(units, w_up, w_down_t):
    blocks = [(u, at, min(at + HID_TILE, u[3][1])) for u in units for at in range(u[3][0], u[3][1], HID_TILE)]
    rows, pre, hidden, totals = {}, {}, {}, {}

    def up(n):
        unit, lo, hi = blocks[n]
        if lo == unit[3][0]:
            rows[id(unit)] = unit[0]().T.astype(jnp.bfloat16)
        pre[n] = jnp.dot(rows[id(unit)], w_up[:, lo:hi], preferred_element_type=jnp.float32)

    def act(n):
        unit, lo, hi = blocks[n]
        hidden[n] = gelu_from_half(pre.pop(n) * unit[1](lo, hi) + unit[2](lo, hi)).astype(jnp.bfloat16)

    def down(n):
        unit, lo, hi = blocks[n]
        part = lax.dot_general(w_down_t[:, lo:hi], hidden.pop(n), (((1,), (1,)), ((), ())),
                               preferred_element_type=jnp.float32)
        totals[id(unit)] = part if lo == unit[3][0] else totals[id(unit)] + part
        if hi == unit[3][1]:
            unit[4](totals.pop(id(unit)))

    for n in range(min(LOOK, len(blocks))):
        up(n)
    for n in range(len(blocks)):
        if n + LOOK < len(blocks):
            up(n + LOOK)
        act(n)
        if n >= LAG:
            down(n - LAG)
    for n in range(max(0, len(blocks) - LAG), len(blocks)):
        down(n)


def kernel(x_ref, up_ref, down_ref, gam_ref, bet_ref, step_ref, out_ref,
           x0, w_own, w_other, rows, steps, w_up, w_down_t, scale, shift, first, final, tally,
           loc_sem, rsend, rrecv, hsend, hrecv, wsend, wrecv, osend, orecv):
    me_m = lax.axis_index("model")
    me_t = lax.axis_index("time")
    me = me_m * NT + me_t
    sample = me // 2
    tok0 = pl.multiple_of((me % 2) * DEV_TOK, DEV_TOK)

    def peer(dm, dt):
        return (0, (me_m + dm) % NM, (me_t + dt) % NT)

    others = [(dm, dt) for dm in range(NM) for dt in range(NT) if (dm, dt) != (0, 0)]

    barrier = pltpu.get_barrier_semaphore()
    for dm, dt in others:
        pl.semaphore_signal(barrier, inc=1, device_id=peer(dm, dt), device_id_type=MESH)

    local = [pltpu.make_async_copy(src, dst, loc_sem.at[n]) for n, (src, dst) in enumerate((
        (gam_ref, rows.at[0, me_t, 0]), (bet_ref, rows.at[0, me_t, 1]), (up_ref, w_own.at[0]), (down_ref, w_own.at[1]),
        (x_ref.at[sample, :, pl.ds(tok0, DEV_TOK)], x0), (step_ref, steps.at[me_t])))]
    for copy in local:
        copy.start()
    keep = pltpu.make_async_copy(x_ref, out_ref.at[0], loc_sem.at[6])

    @pl.when(me_t == 0)
    def _():
        keep.start()

    for copy in local:
        copy.wait()

    def table(half, t, cols, src):
        scale[t, :, cols] = 0.5 * (1.0 + rows[half, t, 0].astype(jnp.float32)[:, src])
        shift[t, :, cols] = 0.5 * rows[half, t, 1].astype(jnp.float32)[:, src]

    own_cols = slice(0, BODY)

    def first_pair(t):
        table(0, t, own_cols, own_cols)

        def unit(r, c):
            tok = slice(c * TM, (c + 1) * TM)

            def done(total):
                first[t, r, :, tok] = total
            return (lambda: x0[:, tok], lambda lo, hi: scale[t, r:r + 1, lo:hi], lambda lo, hi: shift[t, r:r + 1, lo:hi],
                    (0, BODY), done)
        emit([unit(r, c) for r in range(2) for c in range(CHUNKS)], w_up, w_down_t)

    w_up[:, own_cols] = w_own[0][:, own_cols]
    w_down_t[:, own_cols] = w_own[1][:, own_cols]

    @pl.when(me_t < 2)
    def _():
        first_pair(me_t)

    pl.semaphore_wait(barrier, len(others))

    sends = []

    def send(src, dst, ssem, rsem, to):
        copy = pltpu.make_async_remote_copy(src, dst, ssem, rsem, device_id=to, device_id_type=MESH)
        copy.start()
        sends.append(copy)

    def arrived(buf, sem):
        pltpu.make_async_remote_copy(buf, buf, rsend.at[0, 0], sem, device_id=peer(1, 0), device_id_type=MESH).wait_recv()

    mine = rows.at[0, me_t]
    for dt in (2, 3, 1):
        send(mine, mine, rsend.at[0, dt], rrecv.at[0, me_t], peer(0, dt))
    for dt in (2, 3, 1, 0):
        send(mine, rows.at[1, me_t], rsend.at[1, dt], rrecv.at[1, me_t], peer(1, dt))
    send(w_own, w_other, wsend, wrecv, peer(1, 0))
    for dt in (2, 3, 1):
        send(steps.at[me_t], steps.at[me_t], hsend.at[dt], hrecv.at[me_t], peer(0, dt))

    def rows_arrived(half, t):
        if half == 1:
            arrived(rows.at[1, t], rrecv.at[1, t])
        else:
            @pl.when(me_t != t)
            def _():
                arrived(rows.at[0, t], rrecv.at[0, t])

    rows_arrived(0, 0)
    rows_arrived(0, 1)
    first_pair(jnp.where(me_t < 2, 1 - me_t, 0))

    @pl.when(me_t >= 2)
    def _():
        first_pair(1)

    arrived(w_other, wrecv)
    for t in range(NT):
        if t > 1:
            rows_arrived(0, t)
        rows_arrived(1, t)

        @pl.when(me_t != t)
        def _():
            arrived(steps.at[t], hrecv.at[t])

    other_cols = slice(BODY, 2 * BODY)
    rest = slice(BODY, HALF)
    rest_cols = slice(2 * BODY, HIDDEN)

    def join(a, b):
        return jnp.concatenate([a[:, rest], b[:, rest]], axis=1)

    for n, dst in enumerate((w_up, w_down_t)):
        dst[:, other_cols] = w_other[n][:, own_cols]
        dst[:, rest_cols] = join(w_own[n], w_other[n])

    def finish_table(t):
        table(1, t, other_cols, own_cols)
        scale[t, :, rest_cols] = 0.5 * (1.0 + join(rows[0, t, 0].astype(jnp.float32), rows[1, t, 0].astype(jnp.float32)))
        shift[t, :, rest_cols] = 0.5 * join(rows[0, t, 1].astype(jnp.float32), rows[1, t, 1].astype(jnp.float32))

    for t in range(NT):
        if t > 1:
            table(0, t, own_cols, own_cols)
        finish_table(t)

    def step_value(j):
        return steps[j // 2, :, j % 2:j % 2 + 1]

    def place(j, c):
        return out_ref.at[j % 2, sample, :, pl.ds(pl.multiple_of(tok0 + c * TM, TM), TM)]

    def send_latents(first_j, last_j, c):
        owner, count = first_j // 2, last_j - first_j + 1
        src = final.at[c, pl.ds(first_j, count)]
        dst = out_ref.at[pl.ds(first_j % 2, count), sample, :, pl.ds(pl.multiple_of(tok0 + c * TM, TM), TM)]
        pltpu.make_async_remote_copy(src, dst, osend.at[0], orecv.at[0],
                                     device_id=(0, (me_m + 1) % NM, owner), device_id_type=MESH).start()

        @pl.when(me_t != owner)
        def _():
            pltpu.make_async_remote_copy(src, dst, osend.at[1 + owner], orecv.at[0],
                                         device_id=(0, me_m, owner), device_id_type=MESH).start()

    latents = {}
    settled, running = {}, {}

    def unit(sweep, j, c):
        tok = slice(c * TM, (c + 1) * TM)

        def latent():
            return x0[:, tok] if sweep == 1 else latents[sweep - 1, j, c]

        def done(total):
            if sweep == 1:
                total = first[j // 2, j % 2, :, tok] + total
            value = step_value(j) * total
            base = running[c] if j > sweep - 1 else settled.get(c)
            running[c] = value if base is None else base + value
            latents[sweep, j + 1, c] = x0[:, tok] + running[c]
            if j == sweep - 1:
                settled[c] = running[c]
            if j == sweep - 1 or sweep == SWEEPS:
                final[c, j + 1] = latents[sweep, j + 1, c]
                if j + 1 in SEND_AFTER:
                    send_latents(SEND_AFTER[j + 1], j + 1, c)
        row = slice(j % 2, j % 2 + 1)
        return (latent, lambda lo, hi: scale[j // 2, row, lo:hi], lambda lo, hi: shift[j // 2, row, lo:hi],
                (BODY if sweep == 1 else 0, HIDDEN), done)

    emit([unit(sweep, j, c) for c in range(CHUNKS) for sweep in range(1, SWEEPS + 1) for j in range(sweep - 1, sweep + 3)],
         w_up, w_down_t)

    for j in range(1, STEPS):
        @pl.when(me_t == j // 2)
        def _():
            for c in range(CHUNKS):
                place(j, c)[...] = final[c, j]

    for copy in sends:
        copy.wait_send()
    def drained(sem, count):
        pltpu.make_async_copy(tally.at[pl.ds(0, count)], tally.at[pl.ds(0, count)], sem).wait()

    drained(osend.at[0], CHUNKS * (STEPS - 1))
    for owner in range(NT):
        @pl.when(me_t != owner)
        def _():
            drained(osend.at[1 + owner], CHUNKS * (2 if owner else 1))

    @pl.when(me_t == 0)
    def _():
        keep.wait()

    @pl.when(me_t > 0)
    def _():
        drained(orecv.at[0], 2 * CHUNKS * len(others))

    @pl.when(me_t == 0)
    def _():
        drained(orecv.at[0], CHUNKS * len(others))


def solution(mesh):
    def device_body(x_init, w_up, w_down, mod_scale, mod_shift, step_size):
        x_t = jnp.swapaxes(x_init, 1, 2)
        anywhere = pl.BlockSpec(memory_space=pl.ANY)
        out = pl.pallas_call(
            kernel,
            out_shape=pltpu.VMEM((2, BATCH, CHAN, TOKENS), jnp.float32),
            in_specs=[anywhere] * 6,
            out_specs=pl.BlockSpec(memory_space=pltpu.VMEM),
            scratch_shapes=[
                pltpu.VMEM((CHAN, DEV_TOK), jnp.float32),
                pltpu.VMEM((2, CHAN, HALF), jnp.bfloat16),
                pltpu.VMEM((2, CHAN, HALF), jnp.bfloat16),
                pltpu.VMEM((NM, NT, 2, 2, HALF), jnp.bfloat16),
                pltpu.VMEM((NT, 1, 2), jnp.float32),
                pltpu.VMEM((CHAN, HIDDEN), jnp.bfloat16),
                pltpu.VMEM((CHAN, HIDDEN), jnp.bfloat16),
                pltpu.VMEM((NT, 2, HIDDEN), jnp.float32),
                pltpu.VMEM((NT, 2, HIDDEN), jnp.float32),
                pltpu.VMEM((2, 2, CHAN, DEV_TOK), jnp.float32),
                pltpu.VMEM((CHUNKS, STEPS, CHAN, TM), jnp.float32),
                pltpu.VMEM((2 * CHUNKS * (NM * NT - 1), CHAN, TM), jnp.float32),
                pltpu.SemaphoreType.DMA((7,)),
                pltpu.SemaphoreType.DMA((NM, NT)),
                pltpu.SemaphoreType.DMA((NM, NT)),
                pltpu.SemaphoreType.DMA((NT,)),
                pltpu.SemaphoreType.DMA((NT,)),
                pltpu.SemaphoreType.DMA,
                pltpu.SemaphoreType.DMA,
                pltpu.SemaphoreType.DMA((1 + NT,)),
                pltpu.SemaphoreType.DMA((1,)),
            ],
            compiler_params=pltpu.CompilerParams(collective_id=0, has_side_effects=True),
        )(x_t, w_up, w_down.T, mod_scale, mod_shift, step_size.reshape(1, 2))
        return jnp.swapaxes(out, 2, 3)

    return jax.shard_map(device_body, mesh=mesh, in_specs=(P('data', None, None), P(None, 'model'), P('model', None), P('time', 'model'), P('time', 'model'), P('time')), out_specs=P('time', 'data', None, None), check_vma=False)
```

```python
import jax
import jax.numpy as jnp
from jax import lax
from jax.experimental import pallas as pl
from jax.experimental.pallas import tpu as pltpu
from jax.sharding import PartitionSpec as P

MESH = pl.DeviceIdType.MESH
SWEEPS = 4
STEPS = 8
NM, NT = 2, 4
BATCH, TOKENS, CHAN = 4, 1024, 16
HALF = 576
BODY = 512
HIDDEN = 2 * HALF
DEV_TOK = BATCH * TOKENS // (NM * NT)
CHUNKS = 2
TM = DEV_TOK // CHUNKS
HID_TILE = 256
LOOK, LAG = 1, 1
SEND_AFTER = {1: 1, 3: 2, 5: 4, 7: 6}
TANH_LIN = 0.7978845608028654
TANH_CUB = TANH_LIN * 0.044715


def gelu_from_half(half):
    inner = half * ((8.0 * TANH_CUB) * (half * half) + 2.0 * TANH_LIN)
    return half * jnp.tanh(inner) + half


def emit(units, w_up, w_down_t):
    blocks = [(u, at, min(at + HID_TILE, u[3][1])) for u in units for at in range(u[3][0], u[3][1], HID_TILE)]
    rows, pre, hidden, totals = {}, {}, {}, {}

    def up(n):
        unit, lo, hi = blocks[n]
        if lo == unit[3][0]:
            rows[id(unit)] = unit[0]().T.astype(jnp.bfloat16)
        pre[n] = jnp.dot(rows[id(unit)], w_up[:, lo:hi], preferred_element_type=jnp.float32)

    def act(n):
        unit, lo, hi = blocks[n]
        hidden[n] = gelu_from_half(pre.pop(n) * unit[1](lo, hi) + unit[2](lo, hi)).astype(jnp.bfloat16)

    def down(n):
        unit, lo, hi = blocks[n]
        part = lax.dot_general(w_down_t[:, lo:hi], hidden.pop(n), (((1,), (1,)), ((), ())),
                               preferred_element_type=jnp.float32)
        totals[id(unit)] = part if lo == unit[3][0] else totals[id(unit)] + part
        if hi == unit[3][1]:
            unit[4](totals.pop(id(unit)))

    for n in range(min(LOOK, len(blocks))):
        up(n)
    for n in range(len(blocks)):
        if n + LOOK < len(blocks):
            up(n + LOOK)
        act(n)
        if n >= LAG:
            down(n - LAG)
    for n in range(max(0, len(blocks) - LAG), len(blocks)):
        down(n)


def kernel(x_ref, up_ref, down_ref, gam_ref, bet_ref, step_ref, out_ref,
           x0, w_own, w_other, rows, steps, w_up, w_down_t, scale, shift, first, final, tally,
           loc_sem, rsend, rrecv, hsend, hrecv, wsend, wrecv, osend, orecv):
    me_m = lax.axis_index("model")
    me_t = lax.axis_index("time")
    me = me_m * NT + me_t
    sample = me // 2
    tok0 = pl.multiple_of((me % 2) * DEV_TOK, DEV_TOK)

    def peer(dm, dt):
        return (0, (me_m + dm) % NM, (me_t + dt) % NT)

    others = [(dm, dt) for dm in range(NM) for dt in range(NT) if (dm, dt) != (0, 0)]

    barrier = pltpu.get_barrier_semaphore()
    for dm, dt in others:
        pl.semaphore_signal(barrier, inc=1, device_id=peer(dm, dt), device_id_type=MESH)

    local = [pltpu.make_async_copy(src, dst, loc_sem.at[n]) for n, (src, dst) in enumerate((
        (gam_ref, rows.at[0, me_t, 0]), (bet_ref, rows.at[0, me_t, 1]), (up_ref, w_own.at[0]), (down_ref, w_own.at[1]),
        (x_ref.at[sample, :, pl.ds(tok0, DEV_TOK)], x0), (step_ref, steps.at[me_t])))]
    for copy in local:
        copy.start()
    keep = pltpu.make_async_copy(x_ref, out_ref.at[0], loc_sem.at[6])

    @pl.when(me_t == 0)
    def _():
        keep.start()

    for copy in local:
        copy.wait()

    def table(half, t, cols, src):
        scale[t, :, cols] = 0.5 * (1.0 + rows[half, t, 0].astype(jnp.float32)[:, src])
        shift[t, :, cols] = 0.5 * rows[half, t, 1].astype(jnp.float32)[:, src]

    own_cols = slice(0, BODY)

    w_up[:, own_cols] = w_own[0][:, own_cols]
    w_down_t[:, own_cols] = w_own[1][:, own_cols]

    pl.semaphore_wait(barrier, len(others))

    sends = []

    def send(src, dst, ssem, rsem, to):
        copy = pltpu.make_async_remote_copy(src, dst, ssem, rsem, device_id=to, device_id_type=MESH)
        copy.start()
        sends.append(copy)

    def arrived(buf, sem):
        pltpu.make_async_remote_copy(buf, buf, rsend.at[0, 0], sem, device_id=peer(1, 0), device_id_type=MESH).wait_recv()

    mine = rows.at[0, me_t]
    for dt in (2, 3, 1):
        send(mine, mine, rsend.at[0, dt], rrecv.at[0, me_t], peer(0, dt))
    for dt in (2, 3, 1, 0):
        send(mine, rows.at[1, me_t], rsend.at[1, dt], rrecv.at[1, me_t], peer(1, dt))
    send(w_own, w_other, wsend, wrecv, peer(1, 0))
    for dt in (2, 3, 1):
        send(steps.at[me_t], steps.at[me_t], hsend.at[dt], hrecv.at[me_t], peer(0, dt))

    def rows_arrived(half, t):
        if half == 1:
            arrived(rows.at[1, t], rrecv.at[1, t])
        else:
            @pl.when(me_t != t)
            def _():
                arrived(rows.at[0, t], rrecv.at[0, t])

    def first_unit(j, c):
        tok = slice(c * TM, (c + 1) * TM)
        row = slice(j % 2, j % 2 + 1)

        def done(total):
            first[j // 2, j % 2, :, tok] = total
        return (lambda: x0[:, tok], lambda lo, hi: scale[j // 2, row, lo:hi], lambda lo, hi: shift[j // 2, row, lo:hi],
                (0, BODY), done)

    for t in range(2):
        rows_arrived(0, t)
        table(0, t, own_cols, own_cols)
    emit([first_unit(j, c) for j in range(SWEEPS) for c in range(CHUNKS)], w_up, w_down_t)

    arrived(w_other, wrecv)
    for t in range(NT):
        if t > 1:
            rows_arrived(0, t)
        rows_arrived(1, t)

        @pl.when(me_t != t)
        def _():
            arrived(steps.at[t], hrecv.at[t])

    other_cols = slice(BODY, 2 * BODY)
    rest = slice(BODY, HALF)
    rest_cols = slice(2 * BODY, HIDDEN)

    def join(a, b):
        return jnp.concatenate([a[:, rest], b[:, rest]], axis=1)

    for n, dst in enumerate((w_up, w_down_t)):
        dst[:, other_cols] = w_other[n][:, own_cols]
        dst[:, rest_cols] = join(w_own[n], w_other[n])

    def finish_table(t):
        table(1, t, other_cols, own_cols)
        scale[t, :, rest_cols] = 0.5 * (1.0 + join(rows[0, t, 0].astype(jnp.float32), rows[1, t, 0].astype(jnp.float32)))
        shift[t, :, rest_cols] = 0.5 * join(rows[0, t, 1].astype(jnp.float32), rows[1, t, 1].astype(jnp.float32))

    for t in range(NT):
        if t > 1:
            table(0, t, own_cols, own_cols)
        finish_table(t)

    def step_value(j):
        return steps[j // 2, :, j % 2:j % 2 + 1]

    def place(j, c):
        return out_ref.at[j % 2, sample, :, pl.ds(pl.multiple_of(tok0 + c * TM, TM), TM)]

    def send_latents(first_j, last_j, c):
        owner, count = first_j // 2, last_j - first_j + 1
        src = final.at[c, pl.ds(first_j, count)]
        dst = out_ref.at[pl.ds(first_j % 2, count), sample, :, pl.ds(pl.multiple_of(tok0 + c * TM, TM), TM)]
        pltpu.make_async_remote_copy(src, dst, osend.at[0], orecv.at[0],
                                     device_id=(0, (me_m + 1) % NM, owner), device_id_type=MESH).start()

        @pl.when(me_t != owner)
        def _():
            pltpu.make_async_remote_copy(src, dst, osend.at[1 + owner], orecv.at[0],
                                         device_id=(0, me_m, owner), device_id_type=MESH).start()

    latents = {}
    settled, running = {}, {}

    def unit(sweep, j, c):
        tok = slice(c * TM, (c + 1) * TM)

        def latent():
            return x0[:, tok] if sweep == 1 else latents[sweep - 1, j, c]

        def done(total):
            if sweep == 1:
                total = first[j // 2, j % 2, :, tok] + total
            value = step_value(j) * total
            base = running[c] if j > sweep - 1 else settled.get(c)
            running[c] = value if base is None else base + value
            latents[sweep, j + 1, c] = x0[:, tok] + running[c]
            if j == sweep - 1:
                settled[c] = running[c]
            if j == sweep - 1 or sweep == SWEEPS:
                final[c, j + 1] = latents[sweep, j + 1, c]
                if j + 1 in SEND_AFTER:
                    send_latents(SEND_AFTER[j + 1], j + 1, c)
        row = slice(j % 2, j % 2 + 1)
        return (latent, lambda lo, hi: scale[j // 2, row, lo:hi], lambda lo, hi: shift[j // 2, row, lo:hi],
                (BODY if sweep == 1 else 0, HIDDEN), done)

    emit([unit(sweep, j, c) for c in range(CHUNKS) for sweep in range(1, SWEEPS + 1) for j in range(sweep - 1, sweep + 3)],
         w_up, w_down_t)

    for j in range(1, STEPS):
        @pl.when(me_t == j // 2)
        def _():
            for c in range(CHUNKS):
                place(j, c)[...] = final[c, j]

    for copy in sends:
        copy.wait_send()
    def drained(sem, count):
        pltpu.make_async_copy(tally.at[pl.ds(0, count)], tally.at[pl.ds(0, count)], sem).wait()

    drained(osend.at[0], CHUNKS * (STEPS - 1))
    for owner in range(NT):
        @pl.when(me_t != owner)
        def _():
            drained(osend.at[1 + owner], CHUNKS * (2 if owner else 1))

    @pl.when(me_t == 0)
    def _():
        keep.wait()

    @pl.when(me_t > 0)
    def _():
        drained(orecv.at[0], 2 * CHUNKS * len(others))

    @pl.when(me_t == 0)
    def _():
        drained(orecv.at[0], CHUNKS * len(others))


def solution(mesh):
    def device_body(x_init, w_up, w_down, mod_scale, mod_shift, step_size):
        x_t = jnp.swapaxes(x_init, 1, 2)
        anywhere = pl.BlockSpec(memory_space=pl.ANY)
        out = pl.pallas_call(
            kernel,
            out_shape=pltpu.VMEM((2, BATCH, CHAN, TOKENS), jnp.float32),
            in_specs=[anywhere] * 6,
            out_specs=pl.BlockSpec(memory_space=pltpu.VMEM),
            scratch_shapes=[
                pltpu.VMEM((CHAN, DEV_TOK), jnp.float32),
                pltpu.VMEM((2, CHAN, HALF), jnp.bfloat16),
                pltpu.VMEM((2, CHAN, HALF), jnp.bfloat16),
                pltpu.VMEM((NM, NT, 2, 2, HALF), jnp.bfloat16),
                pltpu.VMEM((NT, 1, 2), jnp.float32),
                pltpu.VMEM((CHAN, HIDDEN), jnp.bfloat16),
                pltpu.VMEM((CHAN, HIDDEN), jnp.bfloat16),
                pltpu.VMEM((NT, 2, HIDDEN), jnp.float32),
                pltpu.VMEM((NT, 2, HIDDEN), jnp.float32),
                pltpu.VMEM((2, 2, CHAN, DEV_TOK), jnp.float32),
                pltpu.VMEM((CHUNKS, STEPS, CHAN, TM), jnp.float32),
                pltpu.VMEM((2 * CHUNKS * (NM * NT - 1), CHAN, TM), jnp.float32),
                pltpu.SemaphoreType.DMA((7,)),
                pltpu.SemaphoreType.DMA((NM, NT)),
                pltpu.SemaphoreType.DMA((NM, NT)),
                pltpu.SemaphoreType.DMA((NT,)),
                pltpu.SemaphoreType.DMA((NT,)),
                pltpu.SemaphoreType.DMA,
                pltpu.SemaphoreType.DMA,
                pltpu.SemaphoreType.DMA((1 + NT,)),
                pltpu.SemaphoreType.DMA((1,)),
            ],
            compiler_params=pltpu.CompilerParams(collective_id=0, has_side_effects=True),
        )(x_t, w_up, w_down.T, mod_scale, mod_shift, step_size.reshape(1, 2))
        return jnp.swapaxes(out, 2, 3)

    return jax.shard_map(device_body, mesh=mesh, in_specs=(P('data', None, None), P(None, 'model'), P('model', None), P('time', 'model'), P('time', 'model'), P('time')), out_specs=P('time', 'data', None, None), check_vma=False)
```

```python
import jax
import jax.numpy as jnp
from jax import lax
from jax.experimental import pallas as pl
from jax.experimental.pallas import tpu as pltpu
from jax.sharding import PartitionSpec as P

MESH = pl.DeviceIdType.MESH
SWEEPS = 4
STEPS = 8
NM, NT = 2, 4
BATCH, TOKENS, CHAN = 4, 1024, 16
HALF = 576
BODY = 512
HIDDEN = 2 * HALF
DEV_TOK = BATCH * TOKENS // (NM * NT)
CHUNKS = 2
TM = DEV_TOK // CHUNKS
HID_TILE = 256
LOOK, LAG = 1, 1
SEND_AFTER = {1: 1, 3: 2, 4: 4, 5: 5, 7: 6}
TANH_LIN = 0.7978845608028654
TANH_CUB = TANH_LIN * 0.044715


def gelu_from_half(half):
    inner = half * ((8.0 * TANH_CUB) * (half * half) + 2.0 * TANH_LIN)
    return half * jnp.tanh(inner) + half


def emit(units, w_up, w_down_t):
    blocks = [(u, at, min(at + HID_TILE, u[3][1])) for u in units for at in range(u[3][0], u[3][1], HID_TILE)]
    rows, pre, hidden, totals = {}, {}, {}, {}

    def up(n):
        unit, lo, hi = blocks[n]
        if lo == unit[3][0]:
            rows[id(unit)] = unit[0]().T.astype(jnp.bfloat16)
        pre[n] = jnp.dot(rows[id(unit)], w_up[:, lo:hi], preferred_element_type=jnp.float32)

    def act(n):
        unit, lo, hi = blocks[n]
        hidden[n] = gelu_from_half(pre.pop(n) * unit[1](lo, hi) + unit[2](lo, hi)).astype(jnp.bfloat16)

    def down(n):
        unit, lo, hi = blocks[n]
        part = lax.dot_general(w_down_t[:, lo:hi], hidden.pop(n), (((1,), (1,)), ((), ())),
                               preferred_element_type=jnp.float32)
        totals[id(unit)] = part if lo == unit[3][0] else totals[id(unit)] + part
        if hi == unit[3][1]:
            unit[4](totals.pop(id(unit)))

    for n in range(min(LOOK, len(blocks))):
        up(n)
    for n in range(len(blocks)):
        if n + LOOK < len(blocks):
            up(n + LOOK)
        act(n)
        if n >= LAG:
            down(n - LAG)
    for n in range(max(0, len(blocks) - LAG), len(blocks)):
        down(n)


def kernel(x_ref, up_ref, down_ref, gam_ref, bet_ref, step_ref, out_ref,
           x0, w_own, w_other, rows, steps, w_up, w_down_t, scale, shift, first, final, tally,
           loc_sem, rsend, rrecv, hsend, hrecv, wsend, wrecv, osend, orecv):
    me_m = lax.axis_index("model")
    me_t = lax.axis_index("time")
    me = me_m * NT + me_t
    sample = me // 2
    tok0 = pl.multiple_of((me % 2) * DEV_TOK, DEV_TOK)

    def peer(dm, dt):
        return (0, (me_m + dm) % NM, (me_t + dt) % NT)

    others = [(dm, dt) for dm in range(NM) for dt in range(NT) if (dm, dt) != (0, 0)]

    barrier = pltpu.get_barrier_semaphore()
    for dm, dt in others:
        pl.semaphore_signal(barrier, inc=1, device_id=peer(dm, dt), device_id_type=MESH)

    local = [pltpu.make_async_copy(src, dst, loc_sem.at[n]) for n, (src, dst) in enumerate((
        (gam_ref, rows.at[0, me_t, 0]), (bet_ref, rows.at[0, me_t, 1]), (up_ref, w_own.at[0]), (down_ref, w_own.at[1]),
        (x_ref.at[sample, :, pl.ds(tok0, DEV_TOK)], x0), (step_ref, steps.at[me_t])))]
    for copy in local:
        copy.start()
    keep = pltpu.make_async_copy(x_ref, out_ref.at[0], loc_sem.at[6])

    @pl.when(me_t == 0)
    def _():
        keep.start()

    for copy in local:
        copy.wait()

    def table(half, t, cols, src):
        scale[t, :, cols] = 0.5 * (1.0 + rows[half, t, 0].astype(jnp.float32)[:, src])
        shift[t, :, cols] = 0.5 * rows[half, t, 1].astype(jnp.float32)[:, src]

    own_cols = slice(0, BODY)

    w_up[:, own_cols] = w_own[0][:, own_cols]
    w_down_t[:, own_cols] = w_own[1][:, own_cols]

    pl.semaphore_wait(barrier, len(others))

    sends = []

    def send(src, dst, ssem, rsem, to):
        copy = pltpu.make_async_remote_copy(src, dst, ssem, rsem, device_id=to, device_id_type=MESH)
        copy.start()
        sends.append(copy)

    def arrived(buf, sem):
        pltpu.make_async_remote_copy(buf, buf, rsend.at[0, 0], sem, device_id=peer(1, 0), device_id_type=MESH).wait_recv()

    mine = rows.at[0, me_t]
    for dt in (2, 3, 1):
        send(mine, mine, rsend.at[0, dt], rrecv.at[0, me_t], peer(0, dt))
    for dt in (2, 3, 1, 0):
        send(mine, rows.at[1, me_t], rsend.at[1, dt], rrecv.at[1, me_t], peer(1, dt))
    send(w_own, w_other, wsend, wrecv, peer(1, 0))
    for dt in (2, 3, 1):
        send(steps.at[me_t], steps.at[me_t], hsend.at[dt], hrecv.at[me_t], peer(0, dt))

    def rows_arrived(half, t):
        if half == 1:
            arrived(rows.at[1, t], rrecv.at[1, t])
        else:
            @pl.when(me_t != t)
            def _():
                arrived(rows.at[0, t], rrecv.at[0, t])

    def first_unit(j, c):
        tok = slice(c * TM, (c + 1) * TM)
        row = slice(j % 2, j % 2 + 1)

        def done(total):
            first[j // 2, j % 2, :, tok] = total
        return (lambda: x0[:, tok], lambda lo, hi: scale[j // 2, row, lo:hi], lambda lo, hi: shift[j // 2, row, lo:hi],
                (0, BODY), done)

    for t in range(2):
        rows_arrived(0, t)
        table(0, t, own_cols, own_cols)
    emit([first_unit(j, c) for j in range(SWEEPS) for c in range(CHUNKS)], w_up, w_down_t)

    arrived(w_other, wrecv)
    for t in range(NT):
        if t > 1:
            rows_arrived(0, t)
        rows_arrived(1, t)

        @pl.when(me_t != t)
        def _():
            arrived(steps.at[t], hrecv.at[t])

    other_cols = slice(BODY, 2 * BODY)
    rest = slice(BODY, HALF)
    rest_cols = slice(2 * BODY, HIDDEN)

    def join(a, b):
        return jnp.concatenate([a[:, rest], b[:, rest]], axis=1)

    for n, dst in enumerate((w_up, w_down_t)):
        dst[:, other_cols] = w_other[n][:, own_cols]
        dst[:, rest_cols] = join(w_own[n], w_other[n])

    def finish_table(t):
        table(1, t, other_cols, own_cols)
        scale[t, :, rest_cols] = 0.5 * (1.0 + join(rows[0, t, 0].astype(jnp.float32), rows[1, t, 0].astype(jnp.float32)))
        shift[t, :, rest_cols] = 0.5 * join(rows[0, t, 1].astype(jnp.float32), rows[1, t, 1].astype(jnp.float32))

    for t in range(NT):
        if t > 1:
            table(0, t, own_cols, own_cols)
        finish_table(t)

    def step_value(j):
        return steps[j // 2, :, j % 2:j % 2 + 1]

    def place(j, c):
        return out_ref.at[j % 2, sample, :, pl.ds(pl.multiple_of(tok0 + c * TM, TM), TM)]

    def send_latents(first_j, last_j, c):
        owner, count = first_j // 2, last_j - first_j + 1
        src = final.at[c, pl.ds(first_j, count)]
        dst = out_ref.at[pl.ds(first_j % 2, count), sample, :, pl.ds(pl.multiple_of(tok0 + c * TM, TM), TM)]
        pltpu.make_async_remote_copy(src, dst, osend.at[0], orecv.at[0],
                                     device_id=(0, (me_m + 1) % NM, owner), device_id_type=MESH).start()

        @pl.when(me_t != owner)
        def _():
            pltpu.make_async_remote_copy(src, dst, osend.at[1 + owner], orecv.at[0],
                                         device_id=(0, me_m, owner), device_id_type=MESH).start()

    latents = {}
    settled, running = {}, {}

    def unit(sweep, j, c):
        tok = slice(c * TM, (c + 1) * TM)

        def latent():
            return x0[:, tok] if sweep == 1 else latents[sweep - 1, j, c]

        def done(total):
            if sweep == 1:
                total = first[j // 2, j % 2, :, tok] + total
            value = step_value(j) * total
            base = running[c] if j > sweep - 1 else settled.get(c)
            running[c] = value if base is None else base + value
            latents[sweep, j + 1, c] = x0[:, tok] + running[c]
            if j == sweep - 1:
                settled[c] = running[c]
            if j == sweep - 1 or sweep == SWEEPS:
                final[c, j + 1] = latents[sweep, j + 1, c]
                if j + 1 in SEND_AFTER:
                    send_latents(SEND_AFTER[j + 1], j + 1, c)
        row = slice(j % 2, j % 2 + 1)
        return (latent, lambda lo, hi: scale[j // 2, row, lo:hi], lambda lo, hi: shift[j // 2, row, lo:hi],
                (BODY if sweep == 1 else 0, HIDDEN), done)

    emit([unit(sweep, j, c) for c in range(CHUNKS) for sweep in range(1, SWEEPS + 1) for j in range(sweep - 1, sweep + 3)],
         w_up, w_down_t)

    for j in range(1, STEPS):
        @pl.when(me_t == j // 2)
        def _():
            for c in range(CHUNKS):
                place(j, c)[...] = final[c, j]

    for copy in sends:
        copy.wait_send()
    def drained(sem, count):
        pltpu.make_async_copy(tally.at[pl.ds(0, count)], tally.at[pl.ds(0, count)], sem).wait()

    drained(osend.at[0], CHUNKS * (STEPS - 1))
    for owner in range(NT):
        @pl.when(me_t != owner)
        def _():
            drained(osend.at[1 + owner], CHUNKS * (2 if owner else 1))

    @pl.when(me_t == 0)
    def _():
        keep.wait()

    @pl.when(me_t > 0)
    def _():
        drained(orecv.at[0], 2 * CHUNKS * len(others))

    @pl.when(me_t == 0)
    def _():
        drained(orecv.at[0], CHUNKS * len(others))


def solution(mesh):
    def device_body(x_init, w_up, w_down, mod_scale, mod_shift, step_size):
        x_t = jnp.swapaxes(x_init, 1, 2)
        anywhere = pl.BlockSpec(memory_space=pl.ANY)
        out = pl.pallas_call(
            kernel,
            out_shape=pltpu.VMEM((2, BATCH, CHAN, TOKENS), jnp.float32),
            in_specs=[anywhere] * 6,
            out_specs=pl.BlockSpec(memory_space=pltpu.VMEM),
            scratch_shapes=[
                pltpu.VMEM((CHAN, DEV_TOK), jnp.float32),
                pltpu.VMEM((2, CHAN, HALF), jnp.bfloat16),
                pltpu.VMEM((2, CHAN, HALF), jnp.bfloat16),
                pltpu.VMEM((NM, NT, 2, 2, HALF), jnp.bfloat16),
                pltpu.VMEM((NT, 1, 2), jnp.float32),
                pltpu.VMEM((CHAN, HIDDEN), jnp.bfloat16),
                pltpu.VMEM((CHAN, HIDDEN), jnp.bfloat16),
                pltpu.VMEM((NT, 2, HIDDEN), jnp.float32),
                pltpu.VMEM((NT, 2, HIDDEN), jnp.float32),
                pltpu.VMEM((2, 2, CHAN, DEV_TOK), jnp.float32),
                pltpu.VMEM((CHUNKS, STEPS, CHAN, TM), jnp.float32),
                pltpu.VMEM((2 * CHUNKS * (NM * NT - 1), CHAN, TM), jnp.float32),
                pltpu.SemaphoreType.DMA((7,)),
                pltpu.SemaphoreType.DMA((NM, NT)),
                pltpu.SemaphoreType.DMA((NM, NT)),
                pltpu.SemaphoreType.DMA((NT,)),
                pltpu.SemaphoreType.DMA((NT,)),
                pltpu.SemaphoreType.DMA,
                pltpu.SemaphoreType.DMA,
                pltpu.SemaphoreType.DMA((1 + NT,)),
                pltpu.SemaphoreType.DMA((1,)),
            ],
            compiler_params=pltpu.CompilerParams(collective_id=0, has_side_effects=True),
        )(x_t, w_up, w_down.T, mod_scale, mod_shift, step_size.reshape(1, 2))
        return jnp.swapaxes(out, 2, 3)

    return jax.shard_map(device_body, mesh=mesh, in_specs=(P('data', None, None), P(None, 'model'), P('model', None), P('time', 'model'), P('time', 'model'), P('time')), out_specs=P('time', 'data', None, None), check_vma=False)
```

```python
import jax
import jax.numpy as jnp
from jax import lax
from jax.experimental import pallas as pl
from jax.experimental.pallas import tpu as pltpu
from jax.sharding import PartitionSpec as P

MESH = pl.DeviceIdType.MESH
SWEEPS = 4
STEPS = 8
NM, NT = 2, 4
BATCH, TOKENS, CHAN = 4, 1024, 16
HALF = 576
BODY = 512
HIDDEN = 2 * HALF
DEV_TOK = BATCH * TOKENS // (NM * NT)
CHUNKS = 2
TM = DEV_TOK // CHUNKS
HID_TILE = 256
LOOK, LAG = 1, 1
SEND_AFTER = {1: 1, 3: 2, 4: 4, 5: 5, 7: 6}
TANH_LIN = 0.7978845608028654
TANH_CUB = TANH_LIN * 0.044715


def gelu_from_half(half):
    inner = half * ((8.0 * TANH_CUB) * (half * half) + 2.0 * TANH_LIN)
    return half * jnp.tanh(inner) + half


def emit(units, w_up, w_down_t):
    blocks = [(u, at, min(at + HID_TILE, u[3][1])) for u in units for at in range(u[3][0], u[3][1], HID_TILE)]
    rows, pre, hidden, totals = {}, {}, {}, {}

    def up(n):
        unit, lo, hi = blocks[n]
        if lo == unit[3][0]:
            rows[id(unit)] = unit[0]().T.astype(jnp.bfloat16)
        pre[n] = jnp.dot(rows[id(unit)], w_up[:, lo:hi], preferred_element_type=jnp.float32)

    def act(n):
        unit, lo, hi = blocks[n]
        hidden[n] = gelu_from_half(pre.pop(n) * unit[1](lo, hi) + unit[2](lo, hi)).astype(jnp.bfloat16)

    def down(n):
        unit, lo, hi = blocks[n]
        part = lax.dot_general(w_down_t[:, lo:hi], hidden.pop(n), (((1,), (1,)), ((), ())),
                               preferred_element_type=jnp.float32)
        totals[id(unit)] = part if lo == unit[3][0] else totals[id(unit)] + part
        if hi == unit[3][1]:
            unit[4](totals.pop(id(unit)))

    for n in range(min(LOOK, len(blocks))):
        up(n)
    for n in range(len(blocks)):
        if n + LOOK < len(blocks):
            up(n + LOOK)
        act(n)
        if n >= LAG:
            down(n - LAG)
    for n in range(max(0, len(blocks) - LAG), len(blocks)):
        down(n)


def kernel(x_ref, up_ref, down_ref, gam_ref, bet_ref, step_ref, out_ref,
           x0, w_own, w_other, rows, steps, w_up, w_down_t, scale, shift, first, final, tally,
           loc_sem, rsend, rrecv, hsend, hrecv, wsend, wrecv, osend, orecv):
    me_m = lax.axis_index("model")
    me_t = lax.axis_index("time")
    me = me_m * NT + me_t
    sample = me // 2
    tok0 = pl.multiple_of((me % 2) * DEV_TOK, DEV_TOK)

    def peer(dm, dt):
        return (0, (me_m + dm) % NM, (me_t + dt) % NT)

    others = [(dm, dt) for dm in range(NM) for dt in range(NT) if (dm, dt) != (0, 0)]

    barrier = pltpu.get_barrier_semaphore()
    for dm, dt in others:
        pl.semaphore_signal(barrier, inc=1, device_id=peer(dm, dt), device_id_type=MESH)

    local = [pltpu.make_async_copy(src, dst, loc_sem.at[n]) for n, (src, dst) in enumerate((
        (gam_ref, rows.at[0, me_t, 0]), (bet_ref, rows.at[0, me_t, 1]), (up_ref, w_own.at[0]), (down_ref, w_own.at[1]),
        (x_ref.at[sample, :, pl.ds(tok0, DEV_TOK)], x0), (step_ref, steps.at[me_t])))]
    for copy in local:
        copy.start()
    keep = pltpu.make_async_copy(x_ref, out_ref.at[0], loc_sem.at[6])

    @pl.when(me_t == 0)
    def _():
        keep.start()

    for copy in local:
        copy.wait()

    def table(half, t, cols, src):
        scale[t, :, cols] = 0.5 * (1.0 + rows[half, t, 0].astype(jnp.float32)[:, src])
        shift[t, :, cols] = 0.5 * rows[half, t, 1].astype(jnp.float32)[:, src]

    own_cols = slice(0, BODY)

    w_up[:, own_cols] = w_own[0][:, own_cols]
    w_down_t[:, own_cols] = w_own[1][:, own_cols]

    pl.semaphore_wait(barrier, len(others))

    sends = []

    def send(src, dst, ssem, rsem, to):
        copy = pltpu.make_async_remote_copy(src, dst, ssem, rsem, device_id=to, device_id_type=MESH)
        copy.start()
        sends.append(copy)

    def arrived(buf, sem):
        pltpu.make_async_remote_copy(buf, buf, rsend.at[0, 0], sem, device_id=peer(1, 0), device_id_type=MESH).wait_recv()

    mine = rows.at[0, me_t]
    for dt in (2, 3, 1):
        send(mine, mine, rsend.at[0, dt], rrecv.at[0, me_t], peer(0, dt))
    for dt in (2, 3, 1, 0):
        send(mine, rows.at[1, me_t], rsend.at[1, dt], rrecv.at[1, me_t], peer(1, dt))
    send(w_own, w_other, wsend, wrecv, peer(1, 0))
    for dt in (2, 3, 1):
        send(steps.at[me_t], steps.at[me_t], hsend.at[dt], hrecv.at[me_t], peer(0, dt))

    def rows_arrived(half, t):
        if half == 1:
            arrived(rows.at[1, t], rrecv.at[1, t])
        else:
            @pl.when(me_t != t)
            def _():
                arrived(rows.at[0, t], rrecv.at[0, t])

    def first_unit(j, c):
        tok = slice(c * TM, (c + 1) * TM)
        row = slice(j % 2, j % 2 + 1)

        def done(total):
            first[j // 2, j % 2, :, tok] = total
        return (lambda: x0[:, tok], lambda lo, hi: scale[j // 2, row, lo:hi], lambda lo, hi: shift[j // 2, row, lo:hi],
                (0, BODY), done)

    for t in range(2):
        rows_arrived(0, t)
        table(0, t, own_cols, own_cols)
    emit([first_unit(j, c) for j in range(SWEEPS) for c in range(CHUNKS)], w_up, w_down_t)

    arrived(w_other, wrecv)
    for t in range(NT):
        if t > 1:
            rows_arrived(0, t)
        rows_arrived(1, t)

        @pl.when(me_t != t)
        def _():
            arrived(steps.at[t], hrecv.at[t])

    other_cols = slice(BODY, 2 * BODY)
    rest = slice(BODY, HALF)
    rest_cols = slice(2 * BODY, HIDDEN)

    def join(a, b):
        return jnp.concatenate([a[:, rest], b[:, rest]], axis=1)

    for n, dst in enumerate((w_up, w_down_t)):
        dst[:, other_cols] = w_other[n][:, own_cols]
        dst[:, rest_cols] = join(w_own[n], w_other[n])

    def finish_table(t):
        table(1, t, other_cols, own_cols)
        scale[t, :, rest_cols] = 0.5 * (1.0 + join(rows[0, t, 0].astype(jnp.float32), rows[1, t, 0].astype(jnp.float32)))
        shift[t, :, rest_cols] = 0.5 * join(rows[0, t, 1].astype(jnp.float32), rows[1, t, 1].astype(jnp.float32))

    for t in range(NT):
        if t > 1:
            table(0, t, own_cols, own_cols)
        finish_table(t)

    def step_value(j):
        return steps[j // 2, :, j % 2:j % 2 + 1]

    def place(j, c):
        return out_ref.at[j % 2, sample, :, pl.ds(pl.multiple_of(tok0 + c * TM, TM), TM)]

    def send_latents(first_j, last_j, c):
        owner, count = first_j // 2, last_j - first_j + 1
        src = final.at[c, pl.ds(first_j, count)]
        dst = out_ref.at[pl.ds(first_j % 2, count), sample, :, pl.ds(pl.multiple_of(tok0 + c * TM, TM), TM)]
        pltpu.make_async_remote_copy(src, dst, osend.at[0], orecv.at[0],
                                     device_id=(0, (me_m + 1) % NM, owner), device_id_type=MESH).start()

        @pl.when(me_t != owner)
        def _():
            pltpu.make_async_remote_copy(src, dst, osend.at[1 + owner], orecv.at[0],
                                         device_id=(0, me_m, owner), device_id_type=MESH).start()

    latents = {}
    settled, running = {}, {}

    def unit(sweep, j, c):
        tok = slice(c * TM, (c + 1) * TM)

        def latent():
            return x0[:, tok] if sweep == 1 else latents[sweep - 1, j, c]

        def done(total):
            if sweep == 1:
                total = first[j // 2, j % 2, :, tok] + total
            value = step_value(j) * total
            base = running[c] if j > sweep - 1 else settled.get(c)
            running[c] = value if base is None else base + value
            latents[sweep, j + 1, c] = x0[:, tok] + running[c]
            if j == sweep - 1:
                settled[c] = running[c]
            if j == sweep - 1 or sweep == SWEEPS:
                final[c, j + 1] = latents[sweep, j + 1, c]
                if j + 1 in SEND_AFTER:
                    send_latents(SEND_AFTER[j + 1], j + 1, c)
        row = slice(j % 2, j % 2 + 1)
        return (latent, lambda lo, hi: scale[j // 2, row, lo:hi], lambda lo, hi: shift[j // 2, row, lo:hi],
                (BODY if sweep == 1 else 0, HIDDEN), done)

    emit([unit(1, j, c) for j in range(SWEEPS) for c in range(CHUNKS)]
         + [unit(sweep, j, c) for c in range(CHUNKS) for sweep in range(2, SWEEPS + 1) for j in range(sweep - 1, sweep + 3)],
         w_up, w_down_t)

    for j in range(1, STEPS):
        @pl.when(me_t == j // 2)
        def _():
            for c in range(CHUNKS):
                place(j, c)[...] = final[c, j]

    for copy in sends:
        copy.wait_send()
    def drained(sem, count):
        pltpu.make_async_copy(tally.at[pl.ds(0, count)], tally.at[pl.ds(0, count)], sem).wait()

    drained(osend.at[0], CHUNKS * (STEPS - 1))
    for owner in range(NT):
        @pl.when(me_t != owner)
        def _():
            drained(osend.at[1 + owner], CHUNKS * (2 if owner else 1))

    @pl.when(me_t == 0)
    def _():
        keep.wait()

    @pl.when(me_t > 0)
    def _():
        drained(orecv.at[0], 2 * CHUNKS * len(others))

    @pl.when(me_t == 0)
    def _():
        drained(orecv.at[0], CHUNKS * len(others))


def solution(mesh):
    def device_body(x_init, w_up, w_down, mod_scale, mod_shift, step_size):
        x_t = jnp.swapaxes(x_init, 1, 2)
        anywhere = pl.BlockSpec(memory_space=pl.ANY)
        out = pl.pallas_call(
            kernel,
            out_shape=pltpu.VMEM((2, BATCH, CHAN, TOKENS), jnp.float32),
            in_specs=[anywhere] * 6,
            out_specs=pl.BlockSpec(memory_space=pltpu.VMEM),
            scratch_shapes=[
                pltpu.VMEM((CHAN, DEV_TOK), jnp.float32),
                pltpu.VMEM((2, CHAN, HALF), jnp.bfloat16),
                pltpu.VMEM((2, CHAN, HALF), jnp.bfloat16),
                pltpu.VMEM((NM, NT, 2, 2, HALF), jnp.bfloat16),
                pltpu.VMEM((NT, 1, 2), jnp.float32),
                pltpu.VMEM((CHAN, HIDDEN), jnp.bfloat16),
                pltpu.VMEM((CHAN, HIDDEN), jnp.bfloat16),
                pltpu.VMEM((NT, 2, HIDDEN), jnp.float32),
                pltpu.VMEM((NT, 2, HIDDEN), jnp.float32),
                pltpu.VMEM((2, 2, CHAN, DEV_TOK), jnp.float32),
                pltpu.VMEM((CHUNKS, STEPS, CHAN, TM), jnp.float32),
                pltpu.VMEM((2 * CHUNKS * (NM * NT - 1), CHAN, TM), jnp.float32),
                pltpu.SemaphoreType.DMA((7,)),
                pltpu.SemaphoreType.DMA((NM, NT)),
                pltpu.SemaphoreType.DMA((NM, NT)),
                pltpu.SemaphoreType.DMA((NT,)),
                pltpu.SemaphoreType.DMA((NT,)),
                pltpu.SemaphoreType.DMA,
                pltpu.SemaphoreType.DMA,
                pltpu.SemaphoreType.DMA((1 + NT,)),
                pltpu.SemaphoreType.DMA((1,)),
            ],
            compiler_params=pltpu.CompilerParams(collective_id=0, has_side_effects=True),
        )(x_t, w_up, w_down.T, mod_scale, mod_shift, step_size.reshape(1, 2))
        return jnp.swapaxes(out, 2, 3)

    return jax.shard_map(device_body, mesh=mesh, in_specs=(P('data', None, None), P(None, 'model'), P('model', None), P('time', 'model'), P('time', 'model'), P('time')), out_specs=P('time', 'data', None, None), check_vma=False)
```

```python
import jax
import jax.numpy as jnp
from jax import lax
from jax.experimental import pallas as pl
from jax.experimental.pallas import tpu as pltpu
from jax.sharding import PartitionSpec as P

MESH = pl.DeviceIdType.MESH
SWEEPS = 4
STEPS = 8
NM, NT = 2, 4
BATCH, TOKENS, CHAN = 4, 1024, 16
HALF = 576
BODY = 512
HIDDEN = 2 * HALF
DEV_TOK = BATCH * TOKENS // (NM * NT)
CHUNKS = 2
TM = DEV_TOK // CHUNKS
HID_TILE = 256
LOOK, LAG = 1, 1
SEND_AFTER = {1: 1, 3: 2, 4: 4, 5: 5, 7: 6}
TANH_LIN = 0.7978845608028654
TANH_CUB = TANH_LIN * 0.044715


def gelu_from_half(half):
    inner = half * ((8.0 * TANH_CUB) * (half * half) + 2.0 * TANH_LIN)
    return half * jnp.tanh(inner) + half


def emit(units, w_up, w_down_t):
    blocks = [(u, at, min(at + HID_TILE, u[3][1])) for u in units for at in range(u[3][0], u[3][1], HID_TILE)]
    rows, pre, hidden, totals = {}, {}, {}, {}

    def up(n):
        unit, lo, hi = blocks[n]
        if lo == unit[3][0]:
            rows[id(unit)] = unit[0]().T.astype(jnp.bfloat16)
        pre[n] = jnp.dot(rows[id(unit)], w_up[:, lo:hi], preferred_element_type=jnp.float32)

    def act(n):
        unit, lo, hi = blocks[n]
        hidden[n] = gelu_from_half(pre.pop(n) * unit[1](lo, hi) + unit[2](lo, hi)).astype(jnp.bfloat16)

    def down(n):
        unit, lo, hi = blocks[n]
        part = lax.dot_general(w_down_t[:, lo:hi], hidden.pop(n), (((1,), (1,)), ((), ())),
                               preferred_element_type=jnp.float32)
        totals[id(unit)] = part if lo == unit[3][0] else totals[id(unit)] + part
        if hi == unit[3][1]:
            unit[4](totals.pop(id(unit)))

    for n in range(min(LOOK, len(blocks))):
        up(n)
    for n in range(len(blocks)):
        if n + LOOK < len(blocks):
            up(n + LOOK)
        act(n)
        if n >= LAG:
            down(n - LAG)
    for n in range(max(0, len(blocks) - LAG), len(blocks)):
        down(n)


def kernel(x_ref, up_ref, down_ref, gam_ref, bet_ref, step_ref, out_ref,
           x0, w_own, w_other, rows, steps, w_up, w_down_t, scale, shift, first, final, tally,
           loc_sem, rsend, rrecv, hsend, hrecv, wsend, wrecv, osend, orecv):
    me_m = lax.axis_index("model")
    me_t = lax.axis_index("time")
    me = me_m * NT + me_t
    sample = me // 2
    tok0 = pl.multiple_of((me % 2) * DEV_TOK, DEV_TOK)

    def peer(dm, dt):
        return (0, (me_m + dm) % NM, (me_t + dt) % NT)

    others = [(dm, dt) for dm in range(NM) for dt in range(NT) if (dm, dt) != (0, 0)]

    barrier = pltpu.get_barrier_semaphore()
    for dm, dt in others:
        pl.semaphore_signal(barrier, inc=1, device_id=peer(dm, dt), device_id_type=MESH)

    local = [pltpu.make_async_copy(src, dst, loc_sem.at[n]) for n, (src, dst) in enumerate((
        (gam_ref, rows.at[0, me_t, 0]), (bet_ref, rows.at[0, me_t, 1]), (up_ref, w_own.at[0]), (down_ref, w_own.at[1]),
        (x_ref.at[sample, :, pl.ds(tok0, DEV_TOK)], x0), (step_ref, steps.at[me_t])))]
    for copy in local:
        copy.start()
    keep = pltpu.make_async_copy(x_ref, out_ref.at[0], loc_sem.at[6])

    @pl.when(me_t == 0)
    def _():
        keep.start()

    for copy in local:
        copy.wait()

    def table(half, t, cols, src):
        scale[t, :, cols] = 0.5 * (1.0 + rows[half, t, 0].astype(jnp.float32)[:, src])
        shift[t, :, cols] = 0.5 * rows[half, t, 1].astype(jnp.float32)[:, src]

    own_cols = slice(0, BODY)

    w_up[:, own_cols] = w_own[0][:, own_cols]
    w_down_t[:, own_cols] = w_own[1][:, own_cols]

    pl.semaphore_wait(barrier, len(others))

    sends = []

    def send(src, dst, ssem, rsem, to):
        copy = pltpu.make_async_remote_copy(src, dst, ssem, rsem, device_id=to, device_id_type=MESH)
        copy.start()
        sends.append(copy)

    def arrived(buf, sem):
        pltpu.make_async_remote_copy(buf, buf, rsend.at[0, 0], sem, device_id=peer(1, 0), device_id_type=MESH).wait_recv()

    mine = rows.at[0, me_t]
    for dt in (2, 3, 1):
        send(mine, mine, rsend.at[0, dt], rrecv.at[0, me_t], peer(0, dt))
    for dt in (2, 3, 1, 0):
        send(mine, rows.at[1, me_t], rsend.at[1, dt], rrecv.at[1, me_t], peer(1, dt))
    send(w_own, w_other, wsend, wrecv, peer(1, 0))
    for dt in (2, 3, 1):
        send(steps.at[me_t], steps.at[me_t], hsend.at[dt], hrecv.at[me_t], peer(0, dt))

    def rows_arrived(half, t):
        if half == 1:
            arrived(rows.at[1, t], rrecv.at[1, t])
        else:
            @pl.when(me_t != t)
            def _():
                arrived(rows.at[0, t], rrecv.at[0, t])

    def first_unit(j, c):
        tok = slice(c * TM, (c + 1) * TM)
        row = slice(j % 2, j % 2 + 1)

        def done(total):
            first[j // 2, j % 2, :, tok] = total
        return (lambda: x0[:, tok], lambda lo, hi: scale[j // 2, row, lo:hi], lambda lo, hi: shift[j // 2, row, lo:hi],
                (0, BODY), done)

    for t in range(2):
        rows_arrived(0, t)
        table(0, t, own_cols, own_cols)
    emit([first_unit(j, c) for j in range(SWEEPS) for c in range(CHUNKS)], w_up, w_down_t)

    arrived(w_other, wrecv)
    for t in range(NT):
        if t > 1:
            rows_arrived(0, t)
        rows_arrived(1, t)

        @pl.when(me_t != t)
        def _():
            arrived(steps.at[t], hrecv.at[t])

    other_cols = slice(BODY, 2 * BODY)
    rest = slice(BODY, HALF)
    rest_cols = slice(2 * BODY, HIDDEN)

    def join(a, b):
        return jnp.concatenate([a[:, rest], b[:, rest]], axis=1)

    for n, dst in enumerate((w_up, w_down_t)):
        dst[:, other_cols] = w_other[n][:, own_cols]
        dst[:, rest_cols] = join(w_own[n], w_other[n])

    def finish_table(t):
        table(1, t, other_cols, own_cols)
        scale[t, :, rest_cols] = 0.5 * (1.0 + join(rows[0, t, 0].astype(jnp.float32), rows[1, t, 0].astype(jnp.float32)))
        shift[t, :, rest_cols] = 0.5 * join(rows[0, t, 1].astype(jnp.float32), rows[1, t, 1].astype(jnp.float32))

    for t in range(NT):
        if t > 1:
            table(0, t, own_cols, own_cols)
        finish_table(t)

    def step_value(j):
        return steps[j // 2, :, j % 2:j % 2 + 1]

    def place(j, c):
        return out_ref.at[j % 2, sample, :, pl.ds(pl.multiple_of(tok0 + c * TM, TM), TM)]

    def send_latents(first_j, last_j, c):
        owner, count = first_j // 2, last_j - first_j + 1
        src = final.at[c, pl.ds(first_j, count)]
        dst = out_ref.at[pl.ds(first_j % 2, count), sample, :, pl.ds(pl.multiple_of(tok0 + c * TM, TM), TM)]
        pltpu.make_async_remote_copy(src, dst, osend.at[0], orecv.at[0],
                                     device_id=(0, (me_m + 1) % NM, owner), device_id_type=MESH).start()

        @pl.when(me_t != owner)
        def _():
            pltpu.make_async_remote_copy(src, dst, osend.at[1 + owner], orecv.at[0],
                                         device_id=(0, me_m, owner), device_id_type=MESH).start()

    latents = {}
    settled, running = {}, {}

    def unit(sweep, j, c):
        tok = slice(c * TM, (c + 1) * TM)

        def latent():
            return x0[:, tok] if sweep == 1 else latents[sweep - 1, j, c]

        def done(total):
            if sweep == 1:
                total = first[j // 2, j % 2, :, tok] + total
            value = step_value(j) * total
            base = running[c] if j > sweep - 1 else settled.get(c)
            running[c] = value if base is None else base + value
            latents[sweep, j + 1, c] = x0[:, tok] + running[c]
            if j == sweep - 1:
                settled[c] = running[c]
            if j == sweep - 1 or sweep == SWEEPS:
                final[c, j + 1] = latents[sweep, j + 1, c]
                if j + 1 in SEND_AFTER:
                    send_latents(SEND_AFTER[j + 1], j + 1, c)
        row = slice(j % 2, j % 2 + 1)
        return (latent, lambda lo, hi: scale[j // 2, row, lo:hi], lambda lo, hi: shift[j // 2, row, lo:hi],
                (BODY if sweep == 1 else 0, HIDDEN), done)

    emit([unit(1, j, c) for c in range(CHUNKS) for j in range(SWEEPS)]
         + [unit(sweep, j, c) for c in range(CHUNKS) for sweep in range(2, SWEEPS + 1) for j in range(sweep - 1, sweep + 3)],
         w_up, w_down_t)

    for j in range(1, STEPS):
        @pl.when(me_t == j // 2)
        def _():
            for c in range(CHUNKS):
                place(j, c)[...] = final[c, j]

    for copy in sends:
        copy.wait_send()
    def drained(sem, count):
        pltpu.make_async_copy(tally.at[pl.ds(0, count)], tally.at[pl.ds(0, count)], sem).wait()

    drained(osend.at[0], CHUNKS * (STEPS - 1))
    for owner in range(NT):
        @pl.when(me_t != owner)
        def _():
            drained(osend.at[1 + owner], CHUNKS * (2 if owner else 1))

    @pl.when(me_t == 0)
    def _():
        keep.wait()

    @pl.when(me_t > 0)
    def _():
        drained(orecv.at[0], 2 * CHUNKS * len(others))

    @pl.when(me_t == 0)
    def _():
        drained(orecv.at[0], CHUNKS * len(others))


def solution(mesh):
    def device_body(x_init, w_up, w_down, mod_scale, mod_shift, step_size):
        x_t = jnp.swapaxes(x_init, 1, 2)
        anywhere = pl.BlockSpec(memory_space=pl.ANY)
        out = pl.pallas_call(
            kernel,
            out_shape=pltpu.VMEM((2, BATCH, CHAN, TOKENS), jnp.float32),
            in_specs=[anywhere] * 6,
            out_specs=pl.BlockSpec(memory_space=pltpu.VMEM),
            scratch_shapes=[
                pltpu.VMEM((CHAN, DEV_TOK), jnp.float32),
                pltpu.VMEM((2, CHAN, HALF), jnp.bfloat16),
                pltpu.VMEM((2, CHAN, HALF), jnp.bfloat16),
                pltpu.VMEM((NM, NT, 2, 2, HALF), jnp.bfloat16),
                pltpu.VMEM((NT, 1, 2), jnp.float32),
                pltpu.VMEM((CHAN, HIDDEN), jnp.bfloat16),
                pltpu.VMEM((CHAN, HIDDEN), jnp.bfloat16),
                pltpu.VMEM((NT, 2, HIDDEN), jnp.float32),
                pltpu.VMEM((NT, 2, HIDDEN), jnp.float32),
                pltpu.VMEM((2, 2, CHAN, DEV_TOK), jnp.float32),
                pltpu.VMEM((CHUNKS, STEPS, CHAN, TM), jnp.float32),
                pltpu.VMEM((2 * CHUNKS * (NM * NT - 1), CHAN, TM), jnp.float32),
                pltpu.SemaphoreType.DMA((7,)),
                pltpu.SemaphoreType.DMA((NM, NT)),
                pltpu.SemaphoreType.DMA((NM, NT)),
                pltpu.SemaphoreType.DMA((NT,)),
                pltpu.SemaphoreType.DMA((NT,)),
                pltpu.SemaphoreType.DMA,
                pltpu.SemaphoreType.DMA,
                pltpu.SemaphoreType.DMA((1 + NT,)),
                pltpu.SemaphoreType.DMA((1,)),
            ],
            compiler_params=pltpu.CompilerParams(collective_id=0, has_side_effects=True),
        )(x_t, w_up, w_down.T, mod_scale, mod_shift, step_size.reshape(1, 2))
        return jnp.swapaxes(out, 2, 3)

    return jax.shard_map(device_body, mesh=mesh, in_specs=(P('data', None, None), P(None, 'model'), P('model', None), P('time', 'model'), P('time', 'model'), P('time')), out_specs=P('time', 'data', None, None), check_vma=False)
```
